32 devices in a mesh: seq: 16 (over z, y, core), head: 2 (over x).
Axes of the slice: x: 2, y: 2, z: 4, core: 2. Of those that a mesh axis runs over, the one named last changes fastest.
Arguments:
- tokens: bfloat16 [8192, 1024], P('seq'), may hold values from -24 to 24
- norm_attn: float32 [1024], replicated, may hold values from 0.5 to 1.5
- self_qkv: bfloat16 [3, 1024, 1024], P(None, None, 'head'), may hold values from -4 to 4
- self_out: bfloat16 [1024, 1024], P('head'), may hold values from -0.1875 to 0.1875
- norm_ffn: float32 [1024], replicated, may hold values from 0.5 to 1.5
- ffn_in: bfloat16 [2, 1024, 2816], P(None, None, 'head'), may hold values from -0.1875 to 0.1875
- ffn_out: bfloat16 [2816, 1024], P('head'), may hold values from -0.109375 to 0.109375
- norm_final: float32 [1024], replicated, may hold values from 0.5 to 1.5
- pad_lengths: int32 [16], replicated, may hold values from 64 to 512
- targets: bfloat16 [512, 1024], replicated, may hold values from -8 to 8
- target_lengths: int32 [4], replicated, may hold values from 32 to 128
- norm_cross: float32 [1024], replicated, may hold values from 0.1 to 1.9
- cross_query: bfloat16 [1024, 1024], P(None, 'head'), may hold values from -4 to 4
- cross_kv: bfloat16 [2, 1024, 1024], P(None, None, 'head'), may hold values from -4 to 4
- cross_out: bfloat16 [1024, 1024], P('head'), may hold values from -4 to 4
Outputs:
- encoded: bfloat16 [8192, 1024], P('seq')
- decoded: bfloat16 [512, 1024], replicated
The draws below stay inside these ranges and needn't reach their ends.
All inputs are finite; a program needn't handle non-finite values.
Results may differ from the reference program's by a relative error of at most 0.033.
Values may be sent and summed in bfloat16 or wider, within the bound.
A program may use at most 128 MiB of HBM per device.

```python
import math
import jax
import jax.numpy as jnp
from jax import lax

D = 1024
HEADS = 16
HD = 64
FF = 2816
TOK_DEV = 512
TGT_SEQS = 4
TGT_LEN = 128
TOKENS = 8192
TGT = 512
BLOCKS = 16


def plant_strength():
    return math.sqrt(300.0 * math.sqrt(HD) / D)


def plant_vectors(seed_key):
    base_key = jax.random.fold_in(seed_key, 9001)
    direction = jax.random.normal(jax.random.fold_in(base_key, 1), (D,), jnp.float32)
    direction = direction / jnp.sqrt(jnp.sum(direction * direction))
    target_dir = jax.random.normal(jax.random.fold_in(base_key, 2), (HEADS, HD), jnp.float32)
    target_dir = target_dir / jnp.sqrt(jnp.sum(target_dir * target_dir, axis=1, keepdims=True))
    return (direction, target_dir.reshape(HEADS * HD))


def projection(seed_key, salt, planted):
    matrix = jax.random.normal(jax.random.fold_in(seed_key, salt), (planted.shape[0], D, HEADS * HD), jnp.float32) * D ** (-0.5)
    matrix = jnp.clip(matrix, -3.5, 3.5)
    direction, target_dir = plant_vectors(seed_key)
    bump = plant_strength() * jnp.outer(direction, target_dir)
    matrix = matrix + planted[:, None, None] * bump[None, :, :]
    return matrix


def draw_self_qkv(seed_key, part_index):
    return projection(seed_key, 11, jnp.array([1.0, 1.0, 0.0], jnp.float32)).astype(jnp.bfloat16)


def draw_cross_query(seed_key, part_index):
    return projection(seed_key, 12, jnp.array([1.0], jnp.float32))[0].astype(jnp.bfloat16)


def draw_cross_kv(seed_key, part_index):
    return projection(seed_key, 13, jnp.array([1.0, 0.0], jnp.float32)).astype(jnp.bfloat16)


def draw_tokens(seed_key, part_index):
    rows_drawn = jnp.clip(jax.random.normal(jax.random.fold_in(seed_key, 21), (TOKENS, D), jnp.float32), -6.0, 6.0)
    direction, target_dir = plant_vectors(seed_key)
    row_ids = jnp.arange(TOKENS, dtype=jnp.int32)[:, None]
    picked = (jax.random.randint(jax.random.fold_in(seed_key, 22), (TOKENS, 1), 0, 32) == 0) | (row_ids % (4 * TOK_DEV) == 0)
    planted_rows = 128.0 * direction[None, :] + 96.0 / math.sqrt(D) * rows_drawn
    rows_drawn = jnp.where(picked, planted_rows, rows_drawn)
    return jnp.clip(rows_drawn, -24.0, 24.0).astype(jnp.bfloat16)


def draw_targets(seed_key, part_index):
    rows_drawn = jnp.clip(jax.random.normal(jax.random.fold_in(seed_key, 31), (TGT, D), jnp.float32), -6.0, 6.0)
    direction, target_dir = plant_vectors(seed_key)
    row_ids = jnp.arange(TGT, dtype=jnp.int32)[:, None]
    picked = (jax.random.randint(jax.random.fold_in(seed_key, 32), (TGT, 1), 0, 16) == 0) | (row_ids == 0)
    rows_drawn = jnp.where(picked, 32.0 * direction[None, :], rows_drawn)
    return jnp.clip(rows_drawn, -8.0, 8.0).astype(jnp.bfloat16)


def set_ends(drawn, own_key, smallest, top_value):
    longest = drawn.shape.index(max(drawn.shape))
    spots = []
    for shift in (0, 1):
        where = [jax.random.randint(jax.random.fold_in(own_key, axis), (), 0, length) for axis, length in enumerate(drawn.shape)]
        where[longest] = (where[longest] + shift) % drawn.shape[longest]
        spots.append(tuple(where))
    return drawn.at[spots[0]].set(smallest).at[spots[1]].set(top_value)


def levels(own_key, shape, shards, least, largest):
    def one(axis_at, shards_of):
        steps = jax.random.uniform(jax.random.fold_in(jax.random.fold_in(own_key, 6), axis_at), (shards_of,), jnp.float32, least / len(shards), largest / len(shards))
        return jnp.repeat(jnp.exp(steps), shape[axis_at] // shards_of).reshape((-1,) + (1,) * (len(shape) - axis_at - 1))

    factor_of = one(*shards[0])
    for cut in shards[1:]:
        factor_of = factor_of * one(*cut)
    return factor_of


def scatter_about(stream_key, extent, scale, reach, cuts=(), held_as=jnp.bfloat16):
    loudness = levels(stream_key, extent, cuts, -0.22, 0.18) if cuts else 1.0
    values = jax.random.normal(stream_key, extent, jnp.float32) * scale * loudness
    return jnp.minimum(jnp.maximum(values, -reach), reach).astype(held_as)


def setup_inputs(seed: int = 0) -> dict:
    key_of = jax.random.split(jax.random.key(seed), 16)
    tokens = draw_tokens(jax.random.fold_in(key_of[15], 71), 0)
    norm_attn = jnp.clip(1.0 + 0.1 * jax.random.normal(key_of[1], (D,), jnp.float32), 0.5, 1.5)
    self_qkv = draw_self_qkv(jax.random.fold_in(key_of[15], 71), 0)
    self_out = scatter_about(key_of[3], (HEADS * HD, D), (HEADS * HD) ** -0.5, 0.1875, ((0, 2),))
    norm_ffn = jnp.clip(1.0 + 0.1 * jax.random.normal(key_of[4], (D,), jnp.float32), 0.5, 1.5)
    ffn_in = scatter_about(key_of[5], (2, D, FF), D ** -0.5, 0.1875, ((2, 2),))
    ffn_out = scatter_about(key_of[6], (FF, D), FF ** -0.5, 0.109375, ((0, 2),))
    norm_final = jnp.clip(1.0 + 0.1 * jax.random.normal(key_of[7], (D,), jnp.float32), 0.5, 1.5)
    pad_lengths = set_ends(jax.random.randint(key_of[8], (BLOCKS,), TOK_DEV // 8, TOK_DEV + 1), jax.random.fold_in(key_of[8], 1), TOK_DEV // 8, TOK_DEV).astype(jnp.int32)
    targets = draw_targets(jax.random.fold_in(key_of[15], 71), 0)
    target_lengths = set_ends(jax.random.randint(key_of[10], (TGT_SEQS,), TGT_LEN // 4, TGT_LEN + 1), jax.random.fold_in(key_of[10], 1), TGT_LEN // 4, TGT_LEN).astype(jnp.int32)
    norm_cross = jnp.clip(1.0 + 0.18 * jax.random.normal(key_of[11], (D,), jnp.float32), 0.1, 1.9)
    cross_query = draw_cross_query(jax.random.fold_in(key_of[15], 71), 0)
    cross_kv = draw_cross_kv(jax.random.fold_in(key_of[15], 71), 0)
    cross_out = scatter_about(key_of[14], (HEADS * HD, D), (8.0 / (HEADS * HD) ** 0.5), 4.0, ((0, 2),))
    return {"tokens": tokens, "norm_attn": norm_attn, "self_qkv": self_qkv, "self_out": self_out, "norm_ffn": norm_ffn, "ffn_in": ffn_in, "ffn_out": ffn_out, "norm_final": norm_final, "pad_lengths": pad_lengths, "targets": targets, "target_lengths": target_lengths, "norm_cross": norm_cross, "cross_query": cross_query, "cross_kv": cross_kv, "cross_out": cross_out}


epsilon = 1e-06
masked_score = -1e+30

def rms_norm(values, gain_vector):
    widened = values.astype(jnp.float32)
    return widened * lax.rsqrt(lax.optimization_barrier(jnp.mean(widened * widened, axis=-1, keepdims=True)) + epsilon) * gain_vector.astype(jnp.float32)

def attend(queries, keys, values, live_keys):
    query_count = queries.shape[0]
    key_count = keys.shape[0]
    query_heads = queries.reshape(query_count, HEADS, HD).transpose(1, 0, 2)
    key_heads = keys.reshape(key_count, HEADS, HD).transpose(1, 0, 2)
    value_heads = values.reshape(key_count, HEADS, HD).transpose(1, 0, 2)
    block_rows = math.gcd(query_count, 1024)
    scaling = HD ** (-0.5)

    def one_head(head_parts):
        head_queries, head_keys, head_values = head_parts
        blocked = head_queries.reshape(query_count // block_rows, block_rows, HD)

        def one_block(block_queries):
            scores = jnp.dot(block_queries, head_keys.T, preferred_element_type=jnp.float32) * scaling
            scores = jnp.where(live_keys[None, :], scores, masked_score)
            row_max = lax.optimization_barrier(jnp.max(scores, axis=1, keepdims=True))
            weights = jnp.where(live_keys[None, :], jnp.exp(scores - row_max), 0.0)
            weight_sum = lax.optimization_barrier(jnp.sum(weights, axis=1, keepdims=True))
            mixed_rows = jnp.dot(weights.astype(jnp.bfloat16), head_values, preferred_element_type=jnp.float32)
            return mixed_rows / weight_sum
        return lax.map(one_block, blocked).reshape(query_count, HD)
    per_head = lax.map(one_head, (query_heads, key_heads, value_heads))
    return per_head.transpose(1, 0, 2).reshape(query_count, HEADS * HD).astype(jnp.bfloat16)

def reference(tokens, norm_attn, self_qkv, self_out, norm_ffn, ffn_in, ffn_out, norm_final, pad_lengths, targets, target_lengths, norm_cross, cross_query, cross_kv, cross_out):
    normed = rms_norm(tokens, norm_attn).astype(jnp.bfloat16)
    queries = jnp.dot(normed, self_qkv[0], preferred_element_type=jnp.float32).astype(jnp.bfloat16)
    keys = jnp.dot(normed, self_qkv[1], preferred_element_type=jnp.float32).astype(jnp.bfloat16)
    values = jnp.dot(normed, self_qkv[2], preferred_element_type=jnp.float32).astype(jnp.bfloat16)
    positions = jnp.arange(TOKENS, dtype=jnp.int32)
    live = positions % TOK_DEV < jnp.repeat(pad_lengths, TOK_DEV, total_repeat_length=TOKENS)
    context = attend(queries, keys, values, live)
    hidden_in = tokens.astype(jnp.float32) + jnp.dot(context, self_out, preferred_element_type=jnp.float32)
    ffn_normed = rms_norm(hidden_in, norm_ffn).astype(jnp.bfloat16)
    gate_proj = jnp.dot(ffn_normed, ffn_in[0], preferred_element_type=jnp.float32)
    up_proj = jnp.dot(ffn_normed, ffn_in[1], preferred_element_type=jnp.float32)
    activated = (jax.nn.gelu(gate_proj, approximate=True) * up_proj).astype(jnp.bfloat16)
    final_in = hidden_in + jnp.dot(activated, ffn_out, preferred_element_type=jnp.float32)
    encoded = rms_norm(final_in, norm_final).astype(jnp.bfloat16)
    cross_normed = rms_norm(targets, norm_cross).astype(jnp.bfloat16)
    cross_queries = jnp.dot(cross_normed, cross_query, preferred_element_type=jnp.float32).astype(jnp.bfloat16)
    cross_keys = jnp.dot(encoded, cross_kv[0], preferred_element_type=jnp.float32).astype(jnp.bfloat16)
    cross_values = jnp.dot(encoded, cross_kv[1], preferred_element_type=jnp.float32).astype(jnp.bfloat16)
    cross_context = attend(cross_queries, cross_keys, cross_values, live)
    slots = jnp.arange(TGT, dtype=jnp.int32)
    target_live = slots % TGT_LEN < jnp.repeat(target_lengths, TGT_LEN, total_repeat_length=TGT)
    cross_total = jnp.dot(cross_context, cross_out, preferred_element_type=jnp.float32)
    decoded = (targets.astype(jnp.float32) + jnp.where(target_live[:, None], cross_total, 0.0)).astype(jnp.bfloat16)
    return (encoded, decoded)
```

```python
import functools
import math

import jax
import jax.numpy as jnp
from jax import lax
from jax.experimental import pallas as pl
from jax.experimental.pallas import tpu as pltpu
from jax.sharding import PartitionSpec as P

HD = 64
TOK_DEV = 512
TGT_LEN = 128

epsilon = 1e-06
masked_score = -1e30
MESH = pl.DeviceIdType.MESH


def rms_norm(values, gain_vector):
    widened = values.astype(jnp.float32)
    return (
        widened
        * lax.rsqrt(jnp.mean(widened * widened, axis=-1, keepdims=True) + epsilon)
        * gain_vector
    )


def spread_heads(per_head):
    return jnp.repeat(per_head.T, HD, axis=1)


def greet_all(me, ring):
    barrier = pltpu.get_barrier_semaphore()

    def greet(i, carry):
        pl.semaphore_signal(
            barrier, inc=1, device_id={"seq": lax.rem(me + i, ring)}, device_id_type=MESH
        )
        return carry

    lax.fori_loop(1, ring, greet, 0)
    pl.semaphore_wait(barrier, ring - 1)


def scatter_kernel(ring, share, q_in, kv_in, q_out, kv_out, qs, qr, ks, kr, fs, fr, ls):
    me = lax.axis_index("seq")
    part = kv_in.shape[1]
    mine = pl.ds(pl.multiple_of(lax.rem(me, share) * part, part), part)
    own_q = pltpu.make_async_copy(q_in.at[me], q_out.at[me], ls.at[0])
    own_kv = pltpu.make_async_copy(kv_in.at[me], kv_out.at[me, mine], ls.at[1])
    own_q.start()
    own_kv.start()
    greet_all(me, ring)

    def q_copy(i):
        to = lax.rem(me + i, ring)
        return pltpu.make_async_remote_copy(
            src_ref=q_in.at[to],
            dst_ref=q_out.at[me],
            send_sem=qs.at[i],
            recv_sem=qr.at[i],
            device_id={"seq": to},
            device_id_type=MESH,
        )

    def kv_copy(i):
        to = lax.rem(me + i, ring)
        rows = pl.ds(pl.multiple_of(lax.rem(to, share) * part, part), part)
        return pltpu.make_async_remote_copy(
            src_ref=kv_in.at[to],
            dst_ref=kv_out.at[me, rows],
            send_sem=ks.at[i],
            recv_sem=kr.at[i],
            device_id={"seq": to},
            device_id_type=MESH,
        )

    def forward(i, k):
        origin = lax.rem(me - i + ring, ring)
        slot = lax.rem(me, share)
        to = me - slot + lax.rem(slot + k, share)
        block = kv_out.at[origin, mine]
        return pltpu.make_async_remote_copy(
            src_ref=block,
            dst_ref=block,
            send_sem=fs.at[i, k],
            recv_sem=fr.at[i, k],
            device_id={"seq": to},
            device_id_type=MESH,
        )

    def arrived(i, k):
        slot = lax.rem(me, share)
        giver = me - slot + lax.rem(slot - k + share, share)
        origin = lax.rem(giver - i + ring, ring)
        rows = pl.ds(pl.multiple_of(lax.rem(giver, share) * part, part), part)
        block = kv_out.at[origin, rows]
        return pltpu.make_async_remote_copy(
            src_ref=block,
            dst_ref=block,
            send_sem=fs.at[i, k],
            recv_sem=fr.at[i, k],
            device_id={"seq": giver},
            device_id_type=MESH,
        )

    def send(i, carry):
        kv_copy(i).start()
        q_copy(i).start()
        return carry

    lax.fori_loop(1, ring, send, 0)
    own_kv.wait()
    for k in range(1, share):
        forward(0, k).start()

    def relay(i, carry):
        pltpu.make_async_remote_copy(
            src_ref=kv_in.at[0],
            dst_ref=kv_out.at[lax.rem(me - i + ring, ring), mine],
            send_sem=ks.at[i],
            recv_sem=kr.at[i],
            device_id={"seq": lax.rem(me + i, ring)},
            device_id_type=MESH,
        ).wait_recv()
        for k in range(1, share):
            forward(i, k).start()
        return carry

    lax.fori_loop(1, ring, relay, 0)

    def finish(i, carry):
        pltpu.make_async_remote_copy(
            src_ref=q_in.at[0],
            dst_ref=q_out.at[lax.rem(me - i + ring, ring)],
            send_sem=qs.at[i],
            recv_sem=qr.at[i],
            device_id={"seq": lax.rem(me + i, ring)},
            device_id_type=MESH,
        ).wait_recv()
        q_copy(i).wait_send()
        kv_copy(i).wait_send()
        return carry

    lax.fori_loop(1, ring, finish, 0)

    def drain(i, carry):
        for k in range(1, share):
            arrived(i, k).wait_recv()
            forward(i, k).wait_send()
        return carry

    lax.fori_loop(0, ring, drain, 0)
    own_q.wait()


def scatter_heads(ring, share, q_send, kv_send):
    part = kv_send.shape[1]
    return pl.pallas_call(
        functools.partial(scatter_kernel, ring, share),
        out_shape=(
            jax.ShapeDtypeStruct(q_send.shape, q_send.dtype),
            jax.ShapeDtypeStruct((ring, part * share, 2 * HD), kv_send.dtype),
        ),
        in_specs=[pl.BlockSpec(memory_space=pltpu.VMEM)] * 2,
        out_specs=(pl.BlockSpec(memory_space=pltpu.VMEM),) * 2,
        scratch_shapes=[
            pltpu.SemaphoreType.DMA((ring,)),
            pltpu.SemaphoreType.DMA((ring,)),
            pltpu.SemaphoreType.DMA((ring,)),
            pltpu.SemaphoreType.DMA((ring,)),
            pltpu.SemaphoreType.DMA((ring, share)),
            pltpu.SemaphoreType.DMA((ring, share)),
            pltpu.SemaphoreType.DMA((2,)),
        ],
        compiler_params=pltpu.CompilerParams(collective_id=0, has_side_effects=True),
        name="scatter_heads",
    )(q_send, kv_send)


def exchange_kernel(ring, x_in, x_out, ss, rs, ls):
    me = lax.axis_index("seq")
    own = pltpu.make_async_copy(x_in.at[me], x_out.at[me], ls)
    own.start()
    greet_all(me, ring)

    def outgoing(i):
        to = lax.rem(me + i, ring)
        return pltpu.make_async_remote_copy(
            src_ref=x_in.at[to],
            dst_ref=x_out.at[me],
            send_sem=ss.at[i],
            recv_sem=rs.at[i],
            device_id={"seq": to},
            device_id_type=MESH,
        )

    def send(i, carry):
        outgoing(i).start()
        return carry

    lax.fori_loop(1, ring, send, 0)

    def finish(i, carry):
        pltpu.make_async_remote_copy(
            src_ref=x_in.at[0],
            dst_ref=x_out.at[lax.rem(me - i + ring, ring)],
            send_sem=ss.at[i],
            recv_sem=rs.at[i],
            device_id={"seq": lax.rem(me + i, ring)},
            device_id_type=MESH,
        ).wait_recv()
        outgoing(i).wait_send()
        return carry

    lax.fori_loop(1, ring, finish, 0)
    own.wait()


def exchange(ring, blocks, which):
    return pl.pallas_call(
        functools.partial(exchange_kernel, ring),
        out_shape=jax.ShapeDtypeStruct(blocks.shape, blocks.dtype),
        in_specs=[pl.BlockSpec(memory_space=pltpu.VMEM)],
        out_specs=pl.BlockSpec(memory_space=pltpu.VMEM),
        scratch_shapes=[
            pltpu.SemaphoreType.DMA((ring,)),
            pltpu.SemaphoreType.DMA((ring,)),
            pltpu.SemaphoreType.DMA,
        ],
        compiler_params=pltpu.CompilerParams(collective_id=which, has_side_effects=True),
        name=f"exchange_{which}",
    )(blocks)


def attend_kernel(lengths, q_ref, kv_ref, o_ref, keys, values, count):
    blocks, span, lanes = kv_ref.shape
    tile = span
    queries = q_ref.shape[1]
    lane = lax.broadcasted_iota(jnp.int32, (span, lanes), 1)
    row = lax.broadcasted_iota(jnp.int32, (span, lanes), 0)

    @pl.when(pl.program_id(0) == 0)
    def pack():
        def place(j, start):
            block = kv_ref[j]
            dead = jnp.where(row < lengths[j], 0.0, masked_score).astype(jnp.bfloat16)
            at = pl.ds(pl.multiple_of(start, 16), span)
            keys[at, :] = jnp.where(lane < HD, block, dead)
            values[at, :] = jnp.where(lane < HD, jnp.ones_like(block), block)
            return start + ((lengths[j] + 15) // 16) * 16

        stop = lax.fori_loop(0, blocks, place, 0)
        at = pl.ds(pl.multiple_of(stop, 16), span)
        keys[at, :] = jnp.where(lane < HD, 0.0, masked_score).astype(jnp.bfloat16)
        values[at, :] = jnp.zeros((span, lanes), jnp.bfloat16)
        count[0] = (stop + tile - 1) // tile

    spare = lax.broadcasted_iota(jnp.int32, (HD, queries), 0)
    pick = jnp.where(spare == 0, 1.0, 0.0).astype(jnp.bfloat16)
    q_wide = jnp.concatenate([q_ref[...], pick], axis=0)

    def step(t, state):
        top, mixed = state
        at = pl.ds(pl.multiple_of(t * tile, tile), tile)
        scores = lax.dot_general(
            keys[at, :], q_wide, (((1,), (0,)), ((), ())), preferred_element_type=jnp.float32
        )
        new_top = jnp.maximum(top, jnp.max(scores, axis=0, keepdims=True))
        weights = jnp.exp(scores - new_top).astype(jnp.bfloat16)
        part = lax.dot_general(
            values[at, :], weights, (((0,), (0,)), ((), ())), preferred_element_type=jnp.float32
        )
        return new_top, mixed * jnp.exp(top - new_top) + part

    top, mixed = lax.fori_loop(
        0,
        count[0],
        step,
        (
            jnp.full((1, queries), masked_score, jnp.float32),
            jnp.zeros((lanes, queries), jnp.float32),
        ),
    )
    o_ref[...] = (mixed[HD:, :] / mixed[0:1, :]).astype(jnp.bfloat16)


def attend(q_all, kv_all, pad_lengths):
    blocks, span, lanes = kv_all.shape
    total = q_all.shape[1]
    width = math.gcd(total, 512)
    return pl.pallas_call(
        attend_kernel,
        out_shape=jax.ShapeDtypeStruct((HD, total), jnp.bfloat16),
        grid_spec=pltpu.PrefetchScalarGridSpec(
            num_scalar_prefetch=1,
            grid=(total // width,),
            in_specs=[
                pl.BlockSpec((HD, width), lambda i, lengths: (0, i)),
                pl.BlockSpec((blocks, span, lanes), lambda i, lengths: (0, 0, 0)),
            ],
            out_specs=pl.BlockSpec((HD, width), lambda i, lengths: (0, i)),
            scratch_shapes=[
                pltpu.VMEM(((blocks + 1) * span, lanes), jnp.bfloat16),
                pltpu.VMEM(((blocks + 1) * span, lanes), jnp.bfloat16),
                pltpu.SMEM((1,), jnp.int32),
            ],
        ),
        compiler_params=pltpu.CompilerParams(
            dimension_semantics=("arbitrary",), vmem_limit_bytes=40 * 1024 * 1024
        ),
        name="attend",
    )(pad_lengths, q_all, kv_all)


def feed_forward(normed_in, ffn_in, ffn_out):
    gate_proj = jnp.dot(normed_in, ffn_in[0], preferred_element_type=jnp.float32)
    up_proj = jnp.dot(normed_in, ffn_in[1], preferred_element_type=jnp.float32)
    activated = (jax.nn.gelu(gate_proj, approximate=True) * up_proj).astype(jnp.bfloat16)
    return jnp.dot(activated, ffn_out, preferred_element_type=jnp.float32)


def local(
    ring,
    tokens,
    norm_attn,
    self_qkv,
    self_out,
    norm_ffn,
    ffn_in,
    ffn_out,
    norm_final,
    pad_lengths,
    targets,
    target_lengths,
    norm_cross,
    cross_query,
    cross_kv,
    cross_out,
):
    row_count = tokens.shape[0]
    heads_here = self_qkv.shape[2] // HD
    share = ring // heads_here
    part = row_count // share
    scaling = HD ** (-0.5)
    normed = rms_norm(tokens, norm_attn).astype(jnp.bfloat16)
    q_t = lax.dot_general(
        self_qkv[0], normed, (((0,), (1,)), ((), ())), preferred_element_type=jnp.float32
    ).astype(jnp.bfloat16) * jnp.bfloat16(scaling)
    keys_local = jnp.dot(normed, self_qkv[1], preferred_element_type=jnp.float32).astype(
        jnp.bfloat16
    )
    values_local = jnp.dot(normed, self_qkv[2], preferred_element_type=jnp.float32).astype(
        jnp.bfloat16
    )
    q_send = (
        q_t.reshape(heads_here, HD, share, part).transpose(0, 2, 1, 3).reshape(ring, HD, part)
    )
    kv_local = jnp.concatenate(
        [
            keys_local.reshape(row_count, heads_here, HD),
            values_local.reshape(row_count, heads_here, HD),
        ],
        axis=2,
    )
    kv_send = kv_local.transpose(1, 0, 2).reshape(ring, part, 2 * HD)
    q_got, kv_got = scatter_heads(ring, share, q_send, kv_send)
    q_all = q_got.transpose(1, 0, 2).reshape(HD, ring * part)
    mixed_t = attend(q_all, kv_got, pad_lengths)
    back = mixed_t.reshape(HD, ring, part).transpose(1, 0, 2)
    context_t = (
        exchange(ring, back, 1)
        .reshape(heads_here, share, HD, part)
        .transpose(0, 2, 1, 3)
        .reshape(heads_here * HD, row_count)
    )
    attn_part = lax.dot_general(
        context_t, self_out, (((0,), (0,)), ((), ())), preferred_element_type=jnp.float32
    )
    hidden_in = tokens.astype(jnp.float32) + lax.psum(
        attn_part.astype(jnp.bfloat16), "head"
    ).astype(jnp.float32)
    ffn_normed = rms_norm(hidden_in, norm_ffn).astype(jnp.bfloat16)
    ffn_part = feed_forward(ffn_normed, ffn_in, ffn_out)
    final_in = hidden_in + lax.psum(ffn_part.astype(jnp.bfloat16), "head").astype(jnp.float32)
    encoded = rms_norm(final_in, norm_final).astype(jnp.bfloat16)
    target_rows = targets.shape[0]
    cross_normed = rms_norm(targets, norm_cross).astype(jnp.bfloat16)
    cross_q_t = lax.dot_general(
        cross_query, cross_normed, (((0,), (1,)), ((), ())), preferred_element_type=jnp.float32
    ).astype(jnp.bfloat16) * jnp.bfloat16(scaling)
    cross_keys = jnp.dot(encoded, cross_kv[0], preferred_element_type=jnp.float32).astype(
        jnp.bfloat16
    )
    cross_values = jnp.dot(encoded, cross_kv[1], preferred_element_type=jnp.float32).astype(
        jnp.bfloat16
    )
    my_length = lax.dynamic_slice_in_dim(pad_lengths, lax.axis_index("seq"), 1, 0)
    mixed, top = cross_attend(my_length, cross_q_t, cross_keys, cross_values)
    slice_rows = target_rows // ring
    sent = (
        mixed.reshape(heads_here, 2 * HD, ring, slice_rows)
        .transpose(2, 0, 1, 3)
        .reshape(ring, heads_here * 2 * HD * slice_rows // 512, 512)
    )
    got = exchange(ring, sent, 2).reshape(ring, heads_here, 2 * HD, slice_rows)
    tops = exchange(
        ring,
        jnp.broadcast_to(
            top.reshape(heads_here, 1, ring, slice_rows)
            .transpose(2, 0, 1, 3)
            .reshape(ring, heads_here, slice_rows),
            (ring, heads_here, slice_rows),
        ),
        3,
    ).reshape(ring, heads_here, 1, slice_rows)
    best = jnp.max(tops, axis=0, keepdims=True)
    summed = jnp.sum(got.astype(jnp.float32) * jnp.exp(tops - best), axis=0)
    cross_context = (summed[:, HD:, :] / summed[:, 0:1, :]).astype(jnp.bfloat16)
    cross_context = cross_context.reshape(heads_here * HD, slice_rows)
    cross_part = lax.dot_general(
        cross_context, cross_out, (((0,), (0,)), ((), ())), preferred_element_type=jnp.float32
    )
    cross_total = lax.psum(cross_part.astype(jnp.bfloat16), "head").astype(jnp.float32)
    slots = lax.axis_index("seq") * slice_rows + jnp.arange(slice_rows, dtype=jnp.int32)
    owner = slots // TGT_LEN
    limits = jnp.sum(
        jnp.where(
            owner[:, None] == jnp.arange(target_lengths.shape[0])[None, :],
            target_lengths[None, :],
            0,
        ),
        axis=1,
    )
    target_live = slots % TGT_LEN < limits
    mine = lax.dynamic_slice_in_dim(targets, lax.axis_index("seq") * slice_rows, slice_rows, 0)
    decoded_here = (
        mine.astype(jnp.float32) + jnp.where(target_live[:, None], cross_total, 0.0)
    ).astype(jnp.bfloat16)
    decoded = lax.all_gather(decoded_here, "seq", axis=0, tiled=True)
    return (encoded, decoded)


def cross_kernel(length, q_ref, k_ref, v_ref, o_ref, top_ref):
    rows = k_ref.shape[0]
    queries = q_ref.shape[1]
    live = lax.broadcasted_iota(jnp.int32, (rows, queries), 0) < length[0]
    lane = lax.broadcasted_iota(jnp.int32, (rows, 2 * HD), 1)
    ones = jnp.ones((rows, 2 * HD), jnp.bfloat16)
    for h in range(2):
        own = lane < HD if h == 0 else lane >= HD
        keys = jnp.where(own, k_ref[...], jnp.zeros_like(ones))
        values = jnp.where(own, v_ref[...], ones)
        scores = lax.dot_general(
            keys, q_ref[...], (((1,), (0,)), ((), ())), preferred_element_type=jnp.float32
        )
        scores = jnp.where(live, scores, masked_score)
        top = jnp.max(scores, axis=0, keepdims=True)
        weights = jnp.exp(scores - top).astype(jnp.bfloat16)
        part = lax.dot_general(
            values, weights, (((0,), (0,)), ((), ())), preferred_element_type=jnp.float32
        ).astype(jnp.bfloat16)
        if h == 0:
            o_ref[0, :HD, :] = part[HD:, :]
            o_ref[0, HD:, :] = part[:HD, :]
        else:
            o_ref[1] = part
        top_ref[h] = top


def cross_attend(my_length, q_t, keys, values):
    rows, width = keys.shape
    queries = q_t.shape[1]
    heads = width // HD
    return pl.pallas_call(
        cross_kernel,
        out_shape=(
            jax.ShapeDtypeStruct((heads, 2 * HD, queries), jnp.bfloat16),
            jax.ShapeDtypeStruct((heads, 1, queries), jnp.float32),
        ),
        grid_spec=pltpu.PrefetchScalarGridSpec(
            num_scalar_prefetch=1,
            grid=(heads // 2,),
            in_specs=[
                pl.BlockSpec((2 * HD, queries), lambda i, n: (i, 0)),
                pl.BlockSpec((rows, 2 * HD), lambda i, n: (0, i)),
                pl.BlockSpec((rows, 2 * HD), lambda i, n: (0, i)),
            ],
            out_specs=(
                pl.BlockSpec((2, 2 * HD, queries), lambda i, n: (i, 0, 0)),
                pl.BlockSpec((2, 1, queries), lambda i, n: (i, 0, 0)),
            ),
        ),
        compiler_params=pltpu.CompilerParams(vmem_limit_bytes=32 * 1024 * 1024),
        name="cross_attend",
    )(my_length, q_t, keys, values)


def solution(mesh):
    ring = mesh.shape["seq"]
    placed = (
        P("seq", None),
        P(),
        P(None, None, "head"),
        P("head", None),
        P(),
        P(None, None, "head"),
        P("head", None),
        P(),
        P(),
        P(),
        P(),
        P(),
        P(None, "head"),
        P(None, None, "head"),
        P("head", None),
    )
    return jax.shard_map(
        functools.partial(local, ring),
        mesh=mesh,
        in_specs=placed,
        out_specs=(P("seq", None), P()),
        check_vma=False,
    )
```

```python
import functools
import math

import jax
import jax.numpy as jnp
from jax import lax
from jax.experimental import pallas as pl
from jax.experimental.pallas import tpu as pltpu
from jax.sharding import PartitionSpec as P

HD = 64
TOK_DEV = 512
TGT_LEN = 128

epsilon = 1e-06
masked_score = -1e30
MESH = pl.DeviceIdType.MESH


def rms_norm(values, gain_vector):
    widened = values.astype(jnp.float32)
    return (
        widened
        * lax.rsqrt(jnp.mean(widened * widened, axis=-1, keepdims=True) + epsilon)
        * gain_vector
    )


def spread_heads(per_head):
    return jnp.repeat(per_head.T, HD, axis=1)


def greet_all(ring, sides):
    me = lax.axis_index("seq")
    here = lax.axis_index("head")
    barrier = pltpu.get_barrier_semaphore()

    def greet(i, carry):
        pl.semaphore_signal(
            barrier, inc=1, device_id={"seq": lax.rem(me + i, ring)}, device_id_type=MESH
        )
        return carry

    lax.fori_loop(1, ring, greet, 0)
    for k in range(1, sides):
        pl.semaphore_signal(
            barrier, inc=1, device_id={"head": lax.rem(here + k, sides)}, device_id_type=MESH
        )
    pl.semaphore_wait(barrier, ring - 1 + sides - 1)


def side_copy(sides, k, source, target, send_sem, recv_sem):
    here = lax.axis_index("head")
    return pltpu.make_async_remote_copy(
        src_ref=source,
        dst_ref=target,
        send_sem=send_sem,
        recv_sem=recv_sem,
        device_id={"head": lax.rem(here + k, sides)},
        device_id_type=MESH,
    )


def scatter_kernel(
    ring, share, sides, q_in, kv_in, w_in, q_out, kv_out, w_out, qs, qr, ks, kr, fs, fr, ls, ws, wr
):
    me = lax.axis_index("seq")
    here = lax.axis_index("head")
    part = kv_in.shape[1]
    mine = pl.ds(pl.multiple_of(lax.rem(me, share) * part, part), part)
    own_q = pltpu.make_async_copy(q_in.at[me], q_out.at[me], ls.at[0])
    own_kv = pltpu.make_async_copy(kv_in.at[me], kv_out.at[me, mine], ls.at[1])
    own_q.start()
    own_kv.start()
    own_w = pltpu.make_async_copy(w_in, w_out.at[here], ls.at[2])
    own_w.start()
    greet_all(ring, sides)

    def q_copy(i):
        to = lax.rem(me + i, ring)
        return pltpu.make_async_remote_copy(
            src_ref=q_in.at[to],
            dst_ref=q_out.at[me],
            send_sem=qs.at[i],
            recv_sem=qr.at[i],
            device_id={"seq": to},
            device_id_type=MESH,
        )

    def kv_copy(i):
        to = lax.rem(me + i, ring)
        rows = pl.ds(pl.multiple_of(lax.rem(to, share) * part, part), part)
        return pltpu.make_async_remote_copy(
            src_ref=kv_in.at[to],
            dst_ref=kv_out.at[me, rows],
            send_sem=ks.at[i],
            recv_sem=kr.at[i],
            device_id={"seq": to},
            device_id_type=MESH,
        )

    def forward(i, k):
        origin = lax.rem(me - i + ring, ring)
        slot = lax.rem(me, share)
        to = me - slot + lax.rem(slot + k, share)
        block = kv_out.at[origin, mine]
        return pltpu.make_async_remote_copy(
            src_ref=block,
            dst_ref=block,
            send_sem=fs.at[i, k],
            recv_sem=fr.at[i, k],
            device_id={"seq": to},
            device_id_type=MESH,
        )

    def arrived(i, k):
        slot = lax.rem(me, share)
        giver = me - slot + lax.rem(slot - k + share, share)
        origin = lax.rem(giver - i + ring, ring)
        rows = pl.ds(pl.multiple_of(lax.rem(giver, share) * part, part), part)
        block = kv_out.at[origin, rows]
        return pltpu.make_async_remote_copy(
            src_ref=block,
            dst_ref=block,
            send_sem=fs.at[i, k],
            recv_sem=fr.at[i, k],
            device_id={"seq": giver},
            device_id_type=MESH,
        )

    def send(i, carry):
        kv_copy(i).start()
        q_copy(i).start()
        return carry

    lax.fori_loop(1, ring, send, 0)
    for k in range(1, sides):
        side_copy(sides, k, w_in, w_out.at[here], ws.at[k], wr.at[k]).start()
    own_kv.wait()
    for k in range(1, share):
        forward(0, k).start()

    def relay(i, carry):
        pltpu.make_async_remote_copy(
            src_ref=kv_in.at[0],
            dst_ref=kv_out.at[lax.rem(me - i + ring, ring), mine],
            send_sem=ks.at[i],
            recv_sem=kr.at[i],
            device_id={"seq": lax.rem(me + i, ring)},
            device_id_type=MESH,
        ).wait_recv()
        for k in range(1, share):
            forward(i, k).start()
        return carry

    lax.fori_loop(1, ring, relay, 0)

    def finish(i, carry):
        pltpu.make_async_remote_copy(
            src_ref=q_in.at[0],
            dst_ref=q_out.at[lax.rem(me - i + ring, ring)],
            send_sem=qs.at[i],
            recv_sem=qr.at[i],
            device_id={"seq": lax.rem(me + i, ring)},
            device_id_type=MESH,
        ).wait_recv()
        q_copy(i).wait_send()
        kv_copy(i).wait_send()
        return carry

    lax.fori_loop(1, ring, finish, 0)

    def drain(i, carry):
        for k in range(1, share):
            arrived(i, k).wait_recv()
            forward(i, k).wait_send()
        return carry

    lax.fori_loop(0, ring, drain, 0)
    for k in range(1, sides):
        origin = lax.rem(here - k + sides, sides)
        side_copy(sides, k, w_in, w_out.at[origin], ws.at[k], wr.at[k]).wait()
    own_q.wait()
    own_w.wait()


def scatter_heads(ring, share, sides, q_send, kv_send, weights):
    part = kv_send.shape[1]
    return pl.pallas_call(
        functools.partial(scatter_kernel, ring, share, sides),
        out_shape=(
            jax.ShapeDtypeStruct(q_send.shape, q_send.dtype),
            jax.ShapeDtypeStruct((ring, part * share, 2 * HD), kv_send.dtype),
            jax.ShapeDtypeStruct((sides,) + weights.shape, weights.dtype),
        ),
        in_specs=[pl.BlockSpec(memory_space=pltpu.VMEM)] * 3,
        out_specs=(pl.BlockSpec(memory_space=pltpu.VMEM),) * 3,
        scratch_shapes=[
            pltpu.SemaphoreType.DMA((ring,)),
            pltpu.SemaphoreType.DMA((ring,)),
            pltpu.SemaphoreType.DMA((ring,)),
            pltpu.SemaphoreType.DMA((ring,)),
            pltpu.SemaphoreType.DMA((ring, share)),
            pltpu.SemaphoreType.DMA((ring, share)),
            pltpu.SemaphoreType.DMA((3,)),
            pltpu.SemaphoreType.DMA((sides,)),
            pltpu.SemaphoreType.DMA((sides,)),
        ],
        compiler_params=pltpu.CompilerParams(
            collective_id=0, has_side_effects=True, vmem_limit_bytes=40 * 1024 * 1024
        ),
        name="scatter_heads",
    )(q_send, kv_send, weights)


def norm_rows(values, gain):
    scale = lax.rsqrt(jnp.mean(values * values, axis=-1, keepdims=True) + epsilon)
    return values * scale * gain


def block_kernel(
    ring, share, sides, x_in, w_out, tokens, g_ffn, g_final, up_hbm, down_hbm,
    encoded,
    context, hidden, normed, parts, up, down, ss, rs, fs, fr, ps, pr, ls,
):
    me = lax.axis_index("seq")
    here = lax.axis_index("head")
    heads = ring // share
    rows, width = tokens.shape
    up_load = pltpu.make_async_copy(up_hbm, up, ls.at[0])
    down_load = pltpu.make_async_copy(down_hbm, down, ls.at[1])
    up_load.start()
    down_load.start()

    def place(side, origin):
        return context.at[lax.rem(origin, share), side * heads + lax.div(origin, share)]

    own = pltpu.make_async_copy(x_in.at[me], place(here, me), ls.at[2])
    own.start()
    greet_all(ring, sides)

    def outgoing(i):
        to = lax.rem(me + i, ring)
        return pltpu.make_async_remote_copy(
            src_ref=x_in.at[to],
            dst_ref=place(here, me),
            send_sem=ss.at[i],
            recv_sem=rs.at[i],
            device_id={"seq": to},
            device_id_type=MESH,
        )

    def relay(i, k):
        block = place(here, lax.rem(me - i + ring, ring))
        return side_copy(sides, k, block, block, fs.at[i, k], fr.at[i, k])

    def send(i, carry):
        outgoing(i).start()
        return carry

    lax.fori_loop(1, ring, send, 0)
    own.wait()
    for k in range(1, sides):
        relay(0, k).start()

    def pass_on(i, carry):
        pltpu.make_async_remote_copy(
            src_ref=x_in.at[0],
            dst_ref=place(here, lax.rem(me - i + ring, ring)),
            send_sem=ss.at[i],
            recv_sem=rs.at[i],
            device_id={"seq": lax.rem(me + i, ring)},
            device_id_type=MESH,
        ).wait_recv()
        for k in range(1, sides):
            relay(i, k).start()
        return carry

    lax.fori_loop(1, ring, pass_on, 0)

    def sent(i, carry):
        outgoing(i).wait_send()
        return carry

    lax.fori_loop(1, ring, sent, 0)

    def drain(i, carry):
        for k in range(1, sides):
            relay(i, k).wait_send()
            origin = lax.rem(here - k + sides, sides)
            block = place(origin, lax.rem(me - i + ring, ring))
            side_copy(sides, k, block, block, fs.at[i, k], fr.at[i, k]).wait_recv()
        return carry

    lax.fori_loop(0, ring, drain, 0)
    part = rows // share

    def project(c, carry):
        at = pl.ds(pl.multiple_of(c * part, part), part)
        flat = context[c].reshape(sides * heads * HD, part)
        total = tokens[at, :].astype(jnp.float32) + lax.dot_general(
            flat, w_out[...], (((0,), (0,)), ((), ())), preferred_element_type=jnp.float32
        )
        hidden[at, :] = total
        normed[at, :] = norm_rows(total, g_ffn[...]).astype(jnp.bfloat16)
        return carry

    lax.fori_loop(0, share, project, 0)
    up_load.wait()
    down_load.wait()
    chunk = math.gcd(rows, 128)
    chunks = rows // chunk

    def span(c):
        return pl.ds(pl.multiple_of(c * chunk, chunk), chunk)

    def swap(c, k, side):
        return side_copy(
            sides, k, parts.at[side, span(c)], parts.at[side, span(c)], ps.at[c, k], pr.at[c, k]
        )

    def feed(c, carry):
        x = normed[span(c), :]
        gate = jnp.dot(x, up[0], preferred_element_type=jnp.float32)
        lift = jnp.dot(x, up[1], preferred_element_type=jnp.float32)
        active = (jax.nn.gelu(gate, approximate=True) * lift).astype(jnp.bfloat16)
        parts[here, span(c), :] = jnp.dot(
            active, down[...], preferred_element_type=jnp.float32
        ).astype(jnp.bfloat16)
        for k in range(1, sides):
            swap(c, k, here).start()
        return carry

    lax.fori_loop(0, chunks, feed, 0)

    def close(c, carry):
        for k in range(1, sides):
            swap(c, k, here).wait_send()
            swap(c, k, lax.rem(here - k + sides, sides)).wait_recv()
        total = hidden[span(c), :]
        for side in range(sides):
            total = total + parts[side, span(c), :].astype(jnp.float32)
        encoded[span(c), :] = norm_rows(total, g_final[...]).astype(jnp.bfloat16)
        return carry

    lax.fori_loop(0, chunks, close, 0)


def encoder_block(ring, share, sides, back, w_out, tokens, g_ffn, g_final, ffn_in, ffn_out):
    rows, width = tokens.shape
    chunks = rows // math.gcd(rows, 128)
    vmem = pl.BlockSpec(memory_space=pltpu.VMEM)
    hbm = pl.BlockSpec(memory_space=pl.ANY)
    return pl.pallas_call(
        functools.partial(block_kernel, ring, share, sides),
        out_shape=jax.ShapeDtypeStruct((rows, width), jnp.bfloat16),
        in_specs=[vmem, vmem, vmem, vmem, vmem, hbm, hbm],
        out_specs=vmem,
        scratch_shapes=[
            pltpu.VMEM((share, sides * (ring // share), HD, rows // share), jnp.bfloat16),
            pltpu.VMEM((rows, width), jnp.float32),
            pltpu.VMEM((rows, width), jnp.bfloat16),
            pltpu.VMEM((sides, rows, width), jnp.bfloat16),
            pltpu.VMEM(ffn_in.shape, jnp.bfloat16),
            pltpu.VMEM(ffn_out.shape, jnp.bfloat16),
            pltpu.SemaphoreType.DMA((ring,)),
            pltpu.SemaphoreType.DMA((ring,)),
            pltpu.SemaphoreType.DMA((ring, sides)),
            pltpu.SemaphoreType.DMA((ring, sides)),
            pltpu.SemaphoreType.DMA((chunks, sides)),
            pltpu.SemaphoreType.DMA((chunks, sides)),
            pltpu.SemaphoreType.DMA((3,)),
        ],
        compiler_params=pltpu.CompilerParams(
            collective_id=1, has_side_effects=True, vmem_limit_bytes=50 * 1024 * 1024
        ),
        name="encoder_block",
    )(back, w_out, tokens, g_ffn[None, :], g_final[None, :], ffn_in, ffn_out)


def merge_kernel(
    ring, sides, mixed, stats, w_ref, mine, live, decoded,
    got, got_stats, parts, ms, mr, ts, tr, ps, pr, ds, dr, fs, fr, ls,
):
    me = lax.axis_index("seq")
    here = lax.axis_index("head")
    rows, width = mine.shape
    mate = me + 1 - 2 * lax.rem(me, 2)

    def slab(owner):
        return pl.ds(pl.multiple_of(owner * rows, rows), rows)

    own_mixed = pltpu.make_async_copy(mixed.at[slab(me)], got.at[me], ls.at[0])
    own_stats = pltpu.make_async_copy(stats.at[slab(me)], got_stats.at[me], ls.at[1])
    own_mixed.start()
    own_stats.start()
    greet_all(ring, sides)

    def copies(i, origin):
        to = lax.rem(me + i, ring)
        return (
            pltpu.make_async_remote_copy(
                src_ref=mixed.at[slab(to)],
                dst_ref=got.at[origin],
                send_sem=ms.at[i],
                recv_sem=mr.at[i],
                device_id={"seq": to},
                device_id_type=MESH,
            ),
            pltpu.make_async_remote_copy(
                src_ref=stats.at[slab(to)],
                dst_ref=got_stats.at[origin],
                send_sem=ts.at[i],
                recv_sem=tr.at[i],
                device_id={"seq": to},
                device_id_type=MESH,
            ),
        )

    def send(i, carry):
        for copy in copies(i, me):
            copy.start()
        return carry

    lax.fori_loop(1, ring, send, 0)

    def collect(i, carry):
        for copy in copies(i, lax.rem(me - i + ring, ring)):
            copy.wait()
        return carry

    lax.fori_loop(1, ring, collect, 0)
    own_mixed.wait()
    own_stats.wait()
    heads = w_ref.shape[0] // HD
    seen = got_stats[...]
    best = jnp.max(seen, axis=0, keepdims=True)
    grow = jnp.exp(seen - best)
    sums = pltpu.roll(seen.reshape(ring * rows, 2 * HD), HD, 1).reshape(ring, rows, 2 * HD)
    weight_sum = jnp.sum(grow * sums, axis=0, keepdims=True)
    factor = (grow / weight_sum).reshape(ring * rows, 2 * HD)
    lane = lax.broadcasted_iota(jnp.int32, (2 * HD, heads * HD), 1)
    row = lax.broadcasted_iota(jnp.int32, (2 * HD, heads * HD), 0)
    spread = jnp.where((lane >= row * HD) & (lane < row * HD + HD), 1.0, 0.0)
    factor = jnp.where(
        lax.broadcasted_iota(jnp.int32, factor.shape, 1) < heads, factor, 0.0
    )
    wide = jnp.dot(
        factor, spread, precision=lax.Precision.HIGHEST, preferred_element_type=jnp.float32
    ).reshape(ring, rows, heads * HD)
    context = jnp.sum(got[...].astype(jnp.float32) * wide, axis=0).astype(jnp.bfloat16)
    parts[here] = jnp.dot(context, w_ref[...], preferred_element_type=jnp.float32).astype(
        jnp.bfloat16
    )

    def swap(k, side):
        return side_copy(sides, k, parts.at[side], parts.at[side], ps.at[k], pr.at[k])

    for k in range(1, sides):
        swap(k, here).start()
    for k in range(1, sides):
        swap(k, here).wait_send()
        swap(k, lax.rem(here - k + sides, sides)).wait_recv()
    total = parts[0].astype(jnp.float32)
    for side in range(1, sides):
        total = total + parts[side].astype(jnp.float32)
    decoded[slab(me), :] = (
        mine[...].astype(jnp.float32) + jnp.where(live[...] > 0.0, total, 0.0)
    ).astype(jnp.bfloat16)

    def spread_out(j, owner):
        block = decoded.at[slab(owner)]
        return pltpu.make_async_remote_copy(
            src_ref=block,
            dst_ref=block,
            send_sem=ds.at[j],
            recv_sem=dr.at[j],
            device_id={"seq": lax.rem(me + 2 * j, ring)},
            device_id_type=MESH,
        )

    def hand_over(j, owner):
        block = decoded.at[slab(owner)]
        return pltpu.make_async_remote_copy(
            src_ref=block,
            dst_ref=block,
            send_sem=fs.at[j],
            recv_sem=fr.at[j],
            device_id={"seq": mate},
            device_id_type=MESH,
        )

    def share_out(j, carry):
        spread_out(j, me).start()
        return carry

    lax.fori_loop(1, ring // 2, share_out, 0)
    hand_over(0, me).start()

    def pass_on(j, carry):
        owner = lax.rem(me - 2 * j + ring, ring)
        spread_out(j, owner).wait_recv()
        hand_over(j, owner).start()
        return carry

    lax.fori_loop(1, ring // 2, pass_on, 0)

    def finish(j, carry):
        spread_out(j, me).wait_send()
        return carry

    lax.fori_loop(1, ring // 2, finish, 0)

    def drain(j, carry):
        hand_over(j, lax.rem(me - 2 * j + ring, ring)).wait_send()
        hand_over(j, lax.rem(mate - 2 * j + ring, ring)).wait_recv()
        return carry

    lax.fori_loop(0, ring // 2, drain, 0)


def merge_targets(ring, sides, mixed, stats, weights, mine, live):
    rows, width = mine.shape
    vmem = pl.BlockSpec(memory_space=pltpu.VMEM)
    dma = pltpu.SemaphoreType.DMA
    return pl.pallas_call(
        functools.partial(merge_kernel, ring, sides),
        out_shape=jax.ShapeDtypeStruct((rows * ring, width), jnp.bfloat16),
        in_specs=[vmem] * 5,
        out_specs=vmem,
        scratch_shapes=[
            pltpu.VMEM((ring, rows, mixed.shape[1]), jnp.bfloat16),
            pltpu.VMEM((ring, rows, stats.shape[1]), jnp.float32),
            pltpu.VMEM((sides, rows, width), jnp.bfloat16),
            dma((ring,)),
            dma((ring,)),
            dma((ring,)),
            dma((ring,)),
            dma((sides,)),
            dma((sides,)),
            dma((ring,)),
            dma((ring,)),
            dma((ring,)),
            dma((ring,)),
            dma((2,)),
        ],
        compiler_params=pltpu.CompilerParams(
            collective_id=2, has_side_effects=True, vmem_limit_bytes=40 * 1024 * 1024
        ),
        name="merge_targets",
    )(mixed, stats, weights, mine, live)


def attend_kernel(lengths, q_ref, kv_ref, o_ref, keys, values, count):
    blocks, span, lanes = kv_ref.shape
    tile = span
    queries = q_ref.shape[1]
    lane = lax.broadcasted_iota(jnp.int32, (span, lanes), 1)
    row = lax.broadcasted_iota(jnp.int32, (span, lanes), 0)

    @pl.when(pl.program_id(0) == 0)
    def pack():
        def place(j, start):
            block = kv_ref[j]
            dead = jnp.where(row < lengths[j], 0.0, masked_score).astype(jnp.bfloat16)
            at = pl.ds(pl.multiple_of(start, 16), span)
            keys[at, :] = jnp.where(lane < HD, block, dead)
            values[at, :] = jnp.where(lane < HD, jnp.ones_like(block), block)
            return start + ((lengths[j] + 15) // 16) * 16

        stop = lax.fori_loop(0, blocks, place, 0)
        at = pl.ds(pl.multiple_of(stop, 16), span)
        keys[at, :] = jnp.where(lane < HD, 0.0, masked_score).astype(jnp.bfloat16)
        values[at, :] = jnp.zeros((span, lanes), jnp.bfloat16)
        count[0] = (stop + tile - 1) // tile

    spare = lax.broadcasted_iota(jnp.int32, (HD, queries), 0)
    pick = jnp.where(spare == 0, 1.0, 0.0).astype(jnp.bfloat16)
    q_wide = jnp.concatenate([q_ref[...], pick], axis=0)

    def step(t, state):
        top, mixed = state
        at = pl.ds(pl.multiple_of(t * tile, tile), tile)
        scores = lax.dot_general(
            keys[at, :], q_wide, (((1,), (0,)), ((), ())), preferred_element_type=jnp.float32
        )
        new_top = jnp.maximum(top, jnp.max(scores, axis=0, keepdims=True))
        weights = jnp.exp(scores - new_top).astype(jnp.bfloat16)
        part = lax.dot_general(
            values[at, :], weights, (((0,), (0,)), ((), ())), preferred_element_type=jnp.float32
        )
        return new_top, mixed * jnp.exp(top - new_top) + part

    top, mixed = lax.fori_loop(
        0,
        count[0],
        step,
        (
            jnp.full((1, queries), masked_score, jnp.float32),
            jnp.zeros((lanes, queries), jnp.float32),
        ),
    )
    o_ref[...] = (mixed[HD:, :] / mixed[0:1, :]).astype(jnp.bfloat16)


def attend(q_all, kv_all, pad_lengths):
    blocks, span, lanes = kv_all.shape
    total = q_all.shape[1]
    width = math.gcd(total, 512)
    return pl.pallas_call(
        attend_kernel,
        out_shape=jax.ShapeDtypeStruct((HD, total), jnp.bfloat16),
        grid_spec=pltpu.PrefetchScalarGridSpec(
            num_scalar_prefetch=1,
            grid=(total // width,),
            in_specs=[
                pl.BlockSpec((HD, width), lambda i, lengths: (0, i)),
                pl.BlockSpec((blocks, span, lanes), lambda i, lengths: (0, 0, 0)),
            ],
            out_specs=pl.BlockSpec((HD, width), lambda i, lengths: (0, i)),
            scratch_shapes=[
                pltpu.VMEM(((blocks + 1) * span, lanes), jnp.bfloat16),
                pltpu.VMEM(((blocks + 1) * span, lanes), jnp.bfloat16),
                pltpu.SMEM((1,), jnp.int32),
            ],
        ),
        compiler_params=pltpu.CompilerParams(
            dimension_semantics=("arbitrary",), vmem_limit_bytes=40 * 1024 * 1024
        ),
        name="attend",
    )(pad_lengths, q_all, kv_all)


def local(
    ring,
    sides,
    tokens,
    norm_attn,
    self_qkv,
    self_out,
    norm_ffn,
    ffn_in,
    ffn_out,
    norm_final,
    pad_lengths,
    targets,
    target_lengths,
    norm_cross,
    cross_query,
    cross_kv,
    cross_out,
):
    row_count = tokens.shape[0]
    heads_here = self_qkv.shape[2] // HD
    share = ring // heads_here
    part = row_count // share
    scaling = HD ** (-0.5)
    normed = rms_norm(tokens, norm_attn).astype(jnp.bfloat16)
    q_t = lax.dot_general(
        self_qkv[0], normed, (((0,), (1,)), ((), ())), preferred_element_type=jnp.float32
    ).astype(jnp.bfloat16) * jnp.bfloat16(scaling)
    keys_local = jnp.dot(normed, self_qkv[1], preferred_element_type=jnp.float32).astype(
        jnp.bfloat16
    )
    values_local = jnp.dot(normed, self_qkv[2], preferred_element_type=jnp.float32).astype(
        jnp.bfloat16
    )
    q_send = (
        q_t.reshape(heads_here, HD, share, part).transpose(0, 2, 1, 3).reshape(ring, HD, part)
    )
    kv_local = jnp.concatenate(
        [
            keys_local.reshape(row_count, heads_here, HD),
            values_local.reshape(row_count, heads_here, HD),
        ],
        axis=2,
    )
    kv_send = kv_local.transpose(1, 0, 2).reshape(ring, part, 2 * HD)
    q_got, kv_got, out_all = scatter_heads(ring, share, sides, q_send, kv_send, self_out)
    q_all = q_got.transpose(1, 0, 2).reshape(HD, ring * part)
    mixed_t = attend(q_all, kv_got, pad_lengths)
    back = mixed_t.reshape(HD, ring, part).transpose(1, 0, 2)
    encoded = encoder_block(
        ring,
        share,
        sides,
        back,
        out_all.reshape(-1, out_all.shape[2]),
        tokens,
        norm_ffn,
        norm_final,
        ffn_in,
        ffn_out,
    )
    target_rows = targets.shape[0]
    cross_normed = rms_norm(targets, norm_cross).astype(jnp.bfloat16)
    cross_q = jnp.dot(cross_normed, cross_query, preferred_element_type=jnp.float32).astype(
        jnp.bfloat16
    ) * jnp.bfloat16(scaling)
    cross_keys = jnp.dot(encoded, cross_kv[0], preferred_element_type=jnp.float32).astype(
        jnp.bfloat16
    )
    cross_values = jnp.dot(encoded, cross_kv[1], preferred_element_type=jnp.float32).astype(
        jnp.bfloat16
    )
    my_length = lax.dynamic_slice_in_dim(pad_lengths, lax.axis_index("seq"), 1, 0)
    mixed, stats = cross_attend(my_length, cross_q, cross_keys, cross_values)
    slice_rows = target_rows // ring
    slots = lax.axis_index("seq") * slice_rows + jnp.arange(slice_rows, dtype=jnp.int32)
    owner = slots // TGT_LEN
    limits = jnp.sum(
        jnp.where(
            owner[:, None] == jnp.arange(target_lengths.shape[0])[None, :],
            target_lengths[None, :],
            0,
        ),
        axis=1,
    )
    target_live = slots % TGT_LEN < limits
    mine = lax.dynamic_slice_in_dim(targets, lax.axis_index("seq") * slice_rows, slice_rows, 0)
    live = jnp.broadcast_to(target_live[:, None], mine.shape).astype(jnp.float32)
    decoded = merge_targets(ring, sides, mixed, stats, cross_out, mine, live)
    return (encoded, decoded)


def cross_kernel(length, q_ref, k_ref, v_ref, o_ref, stats):
    i = pl.program_id(0)
    rows = k_ref.shape[0]
    queries = q_ref.shape[0]
    live = lax.broadcasted_iota(jnp.int32, (queries, rows), 1) < length[0]
    lane = lax.broadcasted_iota(jnp.int32, (rows, 2 * HD), 1)
    out_lane = lax.broadcasted_iota(jnp.int32, (queries, 2 * HD), 1)
    ones = jnp.ones((rows, 2 * HD), jnp.bfloat16)

    @pl.when(i == 0)
    def clear():
        stats[...] = jnp.where(out_lane < HD, 0.0, 1.0)

    pieces = []
    for h in range(2):
        own = lane < HD if h == 0 else lane >= HD
        keys = jnp.where(own, k_ref[...], jnp.zeros_like(ones))
        values = jnp.where(own, v_ref[...], ones)
        scores = lax.dot_general(
            q_ref[...], keys, (((1,), (1,)), ((), ())), preferred_element_type=jnp.float32
        )
        scores = jnp.where(live, scores, masked_score)
        top = jnp.max(scores, axis=1, keepdims=True)
        weights = jnp.exp(scores - top).astype(jnp.bfloat16)
        part = jnp.dot(weights, values, preferred_element_type=jnp.float32)
        total = part[:, 2 * HD - 1 :] if h == 0 else part[:, :1]
        stats[...] = jnp.where(
            out_lane == 2 * i + h,
            top,
            jnp.where(out_lane == HD + 2 * i + h, total, stats[...]),
        )
        pieces.append(part)
    o_ref[...] = jnp.where(out_lane < HD, pieces[0], pieces[1]).astype(jnp.bfloat16)


def cross_attend(my_length, q_all, keys, values):
    rows, width = keys.shape
    queries = q_all.shape[0]
    return pl.pallas_call(
        cross_kernel,
        out_shape=(
            jax.ShapeDtypeStruct((queries, width), jnp.bfloat16),
            jax.ShapeDtypeStruct((queries, 2 * HD), jnp.float32),
        ),
        grid_spec=pltpu.PrefetchScalarGridSpec(
            num_scalar_prefetch=1,
            grid=(width // (2 * HD),),
            in_specs=[
                pl.BlockSpec((queries, 2 * HD), lambda i, n: (0, i)),
                pl.BlockSpec((rows, 2 * HD), lambda i, n: (0, i)),
                pl.BlockSpec((rows, 2 * HD), lambda i, n: (0, i)),
            ],
            out_specs=(
                pl.BlockSpec((queries, 2 * HD), lambda i, n: (0, i)),
                pl.BlockSpec((queries, 2 * HD), lambda i, n: (0, 0)),
            ),
        ),
        compiler_params=pltpu.CompilerParams(
            dimension_semantics=("arbitrary",), vmem_limit_bytes=32 * 1024 * 1024
        ),
        name="cross_attend",
    )(my_length, q_all, keys, values)


def solution(mesh):
    ring = mesh.shape["seq"]
    sides = mesh.shape["head"]
    placed = (
        P("seq", None),
        P(),
        P(None, None, "head"),
        P("head", None),
        P(),
        P(None, None, "head"),
        P("head", None),
        P(),
        P(),
        P(),
        P(),
        P(),
        P(None, "head"),
        P(None, None, "head"),
        P("head", None),
    )
    return jax.shard_map(
        functools.partial(local, ring, sides),
        mesh=mesh,
        in_specs=placed,
        out_specs=(P("seq", None), P()),
        check_vma=False,
    )
```

```python
import functools
import math

import jax
import jax.numpy as jnp
from jax import lax
from jax.experimental import pallas as pl
from jax.experimental.pallas import tpu as pltpu
from jax.sharding import PartitionSpec as P

HD = 64
TOK_DEV = 512
TGT_LEN = 128

epsilon = 1e-06
masked_score = -1e30
MESH = pl.DeviceIdType.MESH


def greet_all(ring, sides):
    me = lax.axis_index("seq")
    here = lax.axis_index("head")
    barrier = pltpu.get_barrier_semaphore()

    def greet(i, carry):
        pl.semaphore_signal(
            barrier, inc=1, device_id={"seq": lax.rem(me + i, ring)}, device_id_type=MESH
        )
        return carry

    lax.fori_loop(1, ring, greet, 0)
    for k in range(1, sides):
        pl.semaphore_signal(
            barrier, inc=1, device_id={"head": lax.rem(here + k, sides)}, device_id_type=MESH
        )
    pl.semaphore_wait(barrier, ring - 1 + sides - 1)


def side_copy(sides, k, source, target, send_sem, recv_sem):
    here = lax.axis_index("head")
    return pltpu.make_async_remote_copy(
        src_ref=source,
        dst_ref=target,
        send_sem=send_sem,
        recv_sem=recv_sem,
        device_id={"head": lax.rem(here + k, sides)},
        device_id_type=MESH,
    )


def scatter_kernel(
    ring, share, sides, q_in, kv_in, w_in, targets, g_cross, w_cross,
    q_out, kv_out, w_out, cross_q, qs, qr, ks, kr, fs, fr, ls, ws, wr,
):
    me = lax.axis_index("seq")
    here = lax.axis_index("head")
    part = kv_in.shape[1]
    mine = pl.ds(pl.multiple_of(lax.rem(me, share) * part, part), part)
    own_q = pltpu.make_async_copy(q_in.at[me], q_out.at[me], ls.at[0])
    own_kv = pltpu.make_async_copy(kv_in.at[me], kv_out.at[me, mine], ls.at[1])
    own_q.start()
    own_kv.start()
    own_w = pltpu.make_async_copy(w_in, w_out.at[here], ls.at[2])
    own_w.start()
    greet_all(ring, sides)

    def q_copy(i):
        to = lax.rem(me + i, ring)
        return pltpu.make_async_remote_copy(
            src_ref=q_in.at[to],
            dst_ref=q_out.at[me],
            send_sem=qs.at[i],
            recv_sem=qr.at[i],
            device_id={"seq": to},
            device_id_type=MESH,
        )

    def kv_copy(i):
        to = lax.rem(me + i, ring)
        rows = pl.ds(pl.multiple_of(lax.rem(to, share) * part, part), part)
        return pltpu.make_async_remote_copy(
            src_ref=kv_in.at[to],
            dst_ref=kv_out.at[me, rows],
            send_sem=ks.at[i],
            recv_sem=kr.at[i],
            device_id={"seq": to},
            device_id_type=MESH,
        )

    def forward(i, k):
        origin = lax.rem(me - i + ring, ring)
        slot = lax.rem(me, share)
        to = me - slot + lax.rem(slot + k, share)
        block = kv_out.at[origin, mine]
        return pltpu.make_async_remote_copy(
            src_ref=block,
            dst_ref=block,
            send_sem=fs.at[i, k],
            recv_sem=fr.at[i, k],
            device_id={"seq": to},
            device_id_type=MESH,
        )

    def arrived(i, k):
        slot = lax.rem(me, share)
        giver = me - slot + lax.rem(slot - k + share, share)
        origin = lax.rem(giver - i + ring, ring)
        rows = pl.ds(pl.multiple_of(lax.rem(giver, share) * part, part), part)
        block = kv_out.at[origin, rows]
        return pltpu.make_async_remote_copy(
            src_ref=block,
            dst_ref=block,
            send_sem=fs.at[i, k],
            recv_sem=fr.at[i, k],
            device_id={"seq": giver},
            device_id_type=MESH,
        )

    def send(i, carry):
        kv_copy(i).start()
        q_copy(i).start()
        return carry

    lax.fori_loop(1, ring, send, 0)
    for k in range(1, sides):
        side_copy(sides, k, w_in, w_out.at[here], ws.at[k], wr.at[k]).start()
    own_kv.wait()
    cross_normed = norm_rows(targets[...].astype(jnp.float32), g_cross[...]).astype(jnp.bfloat16)
    cross_q[...] = jnp.dot(
        cross_normed, w_cross[...], preferred_element_type=jnp.float32
    ).astype(jnp.bfloat16) * jnp.bfloat16(HD ** (-0.5))
    for k in range(1, share):
        forward(0, k).start()

    def relay(i, carry):
        pltpu.make_async_remote_copy(
            src_ref=kv_in.at[0],
            dst_ref=kv_out.at[lax.rem(me - i + ring, ring), mine],
            send_sem=ks.at[i],
            recv_sem=kr.at[i],
            device_id={"seq": lax.rem(me + i, ring)},
            device_id_type=MESH,
        ).wait_recv()
        for k in range(1, share):
            forward(i, k).start()
        return carry

    lax.fori_loop(1, ring, relay, 0)

    def finish(i, carry):
        pltpu.make_async_remote_copy(
            src_ref=q_in.at[0],
            dst_ref=q_out.at[lax.rem(me - i + ring, ring)],
            send_sem=qs.at[i],
            recv_sem=qr.at[i],
            device_id={"seq": lax.rem(me + i, ring)},
            device_id_type=MESH,
        ).wait_recv()
        q_copy(i).wait_send()
        kv_copy(i).wait_send()
        return carry

    lax.fori_loop(1, ring, finish, 0)

    def drain(i, carry):
        for k in range(1, share):
            arrived(i, k).wait_recv()
            forward(i, k).wait_send()
        return carry

    lax.fori_loop(0, ring, drain, 0)
    for k in range(1, sides):
        origin = lax.rem(here - k + sides, sides)
        side_copy(sides, k, w_in, w_out.at[origin], ws.at[k], wr.at[k]).wait()
    own_q.wait()
    own_w.wait()


def scatter_heads(ring, share, sides, q_send, kv_send, weights, targets, g_cross, w_cross):
    part = kv_send.shape[1]
    return pl.pallas_call(
        functools.partial(scatter_kernel, ring, share, sides),
        out_shape=(
            jax.ShapeDtypeStruct(q_send.shape, q_send.dtype),
            jax.ShapeDtypeStruct((ring, part * share, 2 * HD), kv_send.dtype),
            jax.ShapeDtypeStruct((sides,) + weights.shape, weights.dtype),
            jax.ShapeDtypeStruct((targets.shape[0], w_cross.shape[1]), jnp.bfloat16),
        ),
        in_specs=[pl.BlockSpec(memory_space=pltpu.VMEM)] * 6,
        out_specs=(pl.BlockSpec(memory_space=pltpu.VMEM),) * 4,
        scratch_shapes=[
            pltpu.SemaphoreType.DMA((ring,)),
            pltpu.SemaphoreType.DMA((ring,)),
            pltpu.SemaphoreType.DMA((ring,)),
            pltpu.SemaphoreType.DMA((ring,)),
            pltpu.SemaphoreType.DMA((ring, share)),
            pltpu.SemaphoreType.DMA((ring, share)),
            pltpu.SemaphoreType.DMA((3,)),
            pltpu.SemaphoreType.DMA((sides,)),
            pltpu.SemaphoreType.DMA((sides,)),
        ],
        compiler_params=pltpu.CompilerParams(
            collective_id=0, has_side_effects=True, vmem_limit_bytes=40 * 1024 * 1024
        ),
        name="scatter_heads",
    )(q_send, kv_send, weights, targets, g_cross[None, :], w_cross)


def norm_rows(values, gain):
    scale = lax.rsqrt(jnp.mean(values * values, axis=-1, keepdims=True) + epsilon)
    return values * scale * gain


def block_kernel(
    ring, share, sides, x_in, w_out, tokens, g_ffn, g_final, up_hbm, down_hbm,
    encoded,
    context, hidden, normed, parts, up, down, ss, rs, fs, fr, ps, pr, ls,
):
    me = lax.axis_index("seq")
    here = lax.axis_index("head")
    heads = ring // share
    rows, width = tokens.shape
    up_load = pltpu.make_async_copy(up_hbm, up, ls.at[0])
    down_load = pltpu.make_async_copy(down_hbm, down, ls.at[1])
    up_load.start()
    down_load.start()

    def place(side, origin):
        return context.at[lax.rem(origin, share), side * heads + lax.div(origin, share)]

    own = pltpu.make_async_copy(x_in.at[me], place(here, me), ls.at[2])
    own.start()
    greet_all(ring, sides)

    def outgoing(i):
        to = lax.rem(me + i, ring)
        return pltpu.make_async_remote_copy(
            src_ref=x_in.at[to],
            dst_ref=place(here, me),
            send_sem=ss.at[i],
            recv_sem=rs.at[i],
            device_id={"seq": to},
            device_id_type=MESH,
        )

    def relay(i, k):
        block = place(here, lax.rem(me - i + ring, ring))
        return side_copy(sides, k, block, block, fs.at[i, k], fr.at[i, k])

    def send(i, carry):
        outgoing(i).start()
        return carry

    lax.fori_loop(1, ring, send, 0)
    own.wait()
    for k in range(1, sides):
        relay(0, k).start()

    def pass_on(i, carry):
        pltpu.make_async_remote_copy(
            src_ref=x_in.at[0],
            dst_ref=place(here, lax.rem(me - i + ring, ring)),
            send_sem=ss.at[i],
            recv_sem=rs.at[i],
            device_id={"seq": lax.rem(me + i, ring)},
            device_id_type=MESH,
        ).wait_recv()
        for k in range(1, sides):
            relay(i, k).start()
        return carry

    lax.fori_loop(1, ring, pass_on, 0)

    def sent(i, carry):
        outgoing(i).wait_send()
        return carry

    lax.fori_loop(1, ring, sent, 0)

    def drain(i, carry):
        for k in range(1, sides):
            relay(i, k).wait_send()
            origin = lax.rem(here - k + sides, sides)
            block = place(origin, lax.rem(me - i + ring, ring))
            side_copy(sides, k, block, block, fs.at[i, k], fr.at[i, k]).wait_recv()
        return carry

    lax.fori_loop(0, ring, drain, 0)
    part = rows // share

    def project(c, carry):
        at = pl.ds(pl.multiple_of(c * part, part), part)
        flat = context[c].reshape(sides * heads * HD, part)
        total = tokens[at, :].astype(jnp.float32) + lax.dot_general(
            flat, w_out[...], (((0,), (0,)), ((), ())), preferred_element_type=jnp.float32
        )
        hidden[at, :] = total
        normed[at, :] = norm_rows(total, g_ffn[...]).astype(jnp.bfloat16)
        return carry

    lax.fori_loop(0, share, project, 0)
    up_load.wait()
    down_load.wait()
    chunk = math.gcd(rows, 128)
    chunks = rows // chunk

    def span(c):
        return pl.ds(pl.multiple_of(c * chunk, chunk), chunk)

    def swap(c, k, side):
        return side_copy(
            sides, k, parts.at[side, span(c)], parts.at[side, span(c)], ps.at[c, k], pr.at[c, k]
        )

    def feed(c, carry):
        x = normed[span(c), :]
        gate = jnp.dot(x, up[0], preferred_element_type=jnp.float32)
        lift = jnp.dot(x, up[1], preferred_element_type=jnp.float32)
        active = (jax.nn.gelu(gate, approximate=True) * lift).astype(jnp.bfloat16)
        parts[here, span(c), :] = jnp.dot(
            active, down[...], preferred_element_type=jnp.float32
        ).astype(jnp.bfloat16)
        for k in range(1, sides):
            swap(c, k, here).start()
        return carry

    lax.fori_loop(0, chunks, feed, 0)

    def close(c, carry):
        for k in range(1, sides):
            swap(c, k, here).wait_send()
            swap(c, k, lax.rem(here - k + sides, sides)).wait_recv()
        total = hidden[span(c), :]
        for side in range(sides):
            total = total + parts[side, span(c), :].astype(jnp.float32)
        encoded[span(c), :] = norm_rows(total, g_final[...]).astype(jnp.bfloat16)
        return carry

    lax.fori_loop(0, chunks, close, 0)


def encoder_block(ring, share, sides, back, w_out, tokens, g_ffn, g_final, ffn_in, ffn_out):
    rows, width = tokens.shape
    chunks = rows // math.gcd(rows, 128)
    vmem = pl.BlockSpec(memory_space=pltpu.VMEM)
    hbm = pl.BlockSpec(memory_space=pl.ANY)
    return pl.pallas_call(
        functools.partial(block_kernel, ring, share, sides),
        out_shape=jax.ShapeDtypeStruct((rows, width), jnp.bfloat16),
        in_specs=[vmem, vmem, vmem, vmem, vmem, hbm, hbm],
        out_specs=vmem,
        scratch_shapes=[
            pltpu.VMEM((share, sides * (ring // share), HD, rows // share), jnp.bfloat16),
            pltpu.VMEM((rows, width), jnp.float32),
            pltpu.VMEM((rows, width), jnp.bfloat16),
            pltpu.VMEM((sides, rows, width), jnp.bfloat16),
            pltpu.VMEM(ffn_in.shape, jnp.bfloat16),
            pltpu.VMEM(ffn_out.shape, jnp.bfloat16),
            pltpu.SemaphoreType.DMA((ring,)),
            pltpu.SemaphoreType.DMA((ring,)),
            pltpu.SemaphoreType.DMA((ring, sides)),
            pltpu.SemaphoreType.DMA((ring, sides)),
            pltpu.SemaphoreType.DMA((chunks, sides)),
            pltpu.SemaphoreType.DMA((chunks, sides)),
            pltpu.SemaphoreType.DMA((3,)),
        ],
        compiler_params=pltpu.CompilerParams(
            collective_id=1, has_side_effects=True, vmem_limit_bytes=50 * 1024 * 1024
        ),
        name="encoder_block",
    )(back, w_out, tokens, g_ffn[None, :], g_final[None, :], ffn_in, ffn_out)


def merge_kernel(
    ring, sides, mixed, stats, w_ref, mine, live, decoded,
    got, got_stats, parts, ms, mr, ts, tr, ps, pr, ds, dr, fs, fr, ls,
):
    me = lax.axis_index("seq")
    here = lax.axis_index("head")
    rows, width = mine.shape
    mate = me + 1 - 2 * lax.rem(me, 2)

    def slab(owner):
        return pl.ds(pl.multiple_of(owner * rows, rows), rows)

    own_mixed = pltpu.make_async_copy(mixed.at[slab(me)], got.at[me], ls.at[0])
    own_stats = pltpu.make_async_copy(stats.at[slab(me)], got_stats.at[me], ls.at[1])
    own_mixed.start()
    own_stats.start()
    greet_all(ring, sides)

    def copies(i, origin):
        to = lax.rem(me + i, ring)
        return (
            pltpu.make_async_remote_copy(
                src_ref=mixed.at[slab(to)],
                dst_ref=got.at[origin],
                send_sem=ms.at[i],
                recv_sem=mr.at[i],
                device_id={"seq": to},
                device_id_type=MESH,
            ),
            pltpu.make_async_remote_copy(
                src_ref=stats.at[slab(to)],
                dst_ref=got_stats.at[origin],
                send_sem=ts.at[i],
                recv_sem=tr.at[i],
                device_id={"seq": to},
                device_id_type=MESH,
            ),
        )

    def send(i, carry):
        for copy in copies(i, me):
            copy.start()
        return carry

    lax.fori_loop(1, ring, send, 0)

    def collect(i, carry):
        for copy in copies(i, lax.rem(me - i + ring, ring)):
            copy.wait()
        return carry

    lax.fori_loop(1, ring, collect, 0)
    own_mixed.wait()
    own_stats.wait()
    heads = w_ref.shape[0] // HD
    seen = got_stats[...]
    best = jnp.max(seen, axis=0, keepdims=True)
    grow = jnp.exp(seen - best)
    sums = pltpu.roll(seen.reshape(ring * rows, 2 * HD), HD, 1).reshape(ring, rows, 2 * HD)
    weight_sum = jnp.sum(grow * sums, axis=0, keepdims=True)
    factor = (grow / weight_sum).reshape(ring * rows, 2 * HD)
    lane = lax.broadcasted_iota(jnp.int32, (2 * HD, heads * HD), 1)
    row = lax.broadcasted_iota(jnp.int32, (2 * HD, heads * HD), 0)
    spread = jnp.where((lane >= row * HD) & (lane < row * HD + HD), 1.0, 0.0)
    factor = jnp.where(
        lax.broadcasted_iota(jnp.int32, factor.shape, 1) < heads, factor, 0.0
    )
    wide = jnp.dot(
        factor, spread, precision=lax.Precision.HIGHEST, preferred_element_type=jnp.float32
    ).reshape(ring, rows, heads * HD)
    context = jnp.sum(got[...].astype(jnp.float32) * wide, axis=0).astype(jnp.bfloat16)
    parts[here] = jnp.dot(context, w_ref[...], preferred_element_type=jnp.float32).astype(
        jnp.bfloat16
    )

    def swap(k, side):
        return side_copy(sides, k, parts.at[side], parts.at[side], ps.at[k], pr.at[k])

    for k in range(1, sides):
        swap(k, here).start()
    for k in range(1, sides):
        swap(k, here).wait_send()
        swap(k, lax.rem(here - k + sides, sides)).wait_recv()
    total = parts[0].astype(jnp.float32)
    for side in range(1, sides):
        total = total + parts[side].astype(jnp.float32)
    decoded[slab(me), :] = (
        mine[...].astype(jnp.float32) + jnp.where(live[...] > 0.0, total, 0.0)
    ).astype(jnp.bfloat16)

    def spread_out(j, owner):
        block = decoded.at[slab(owner)]
        return pltpu.make_async_remote_copy(
            src_ref=block,
            dst_ref=block,
            send_sem=ds.at[j],
            recv_sem=dr.at[j],
            device_id={"seq": lax.rem(me + 2 * j, ring)},
            device_id_type=MESH,
        )

    def hand_over(j, owner):
        block = decoded.at[slab(owner)]
        return pltpu.make_async_remote_copy(
            src_ref=block,
            dst_ref=block,
            send_sem=fs.at[j],
            recv_sem=fr.at[j],
            device_id={"seq": mate},
            device_id_type=MESH,
        )

    def share_out(j, carry):
        spread_out(j, me).start()
        return carry

    lax.fori_loop(1, ring // 2, share_out, 0)
    hand_over(0, me).start()

    def pass_on(j, carry):
        owner = lax.rem(me - 2 * j + ring, ring)
        spread_out(j, owner).wait_recv()
        hand_over(j, owner).start()
        return carry

    lax.fori_loop(1, ring // 2, pass_on, 0)

    def finish(j, carry):
        spread_out(j, me).wait_send()
        return carry

    lax.fori_loop(1, ring // 2, finish, 0)

    def drain(j, carry):
        hand_over(j, lax.rem(me - 2 * j + ring, ring)).wait_send()
        hand_over(j, lax.rem(mate - 2 * j + ring, ring)).wait_recv()
        return carry

    lax.fori_loop(0, ring // 2, drain, 0)


def merge_targets(ring, sides, mixed, stats, weights, mine, live):
    rows, width = mine.shape
    vmem = pl.BlockSpec(memory_space=pltpu.VMEM)
    dma = pltpu.SemaphoreType.DMA
    return pl.pallas_call(
        functools.partial(merge_kernel, ring, sides),
        out_shape=jax.ShapeDtypeStruct((rows * ring, width), jnp.bfloat16),
        in_specs=[vmem] * 5,
        out_specs=vmem,
        scratch_shapes=[
            pltpu.VMEM((ring, rows, mixed.shape[1]), jnp.bfloat16),
            pltpu.VMEM((ring, rows, stats.shape[1]), jnp.float32),
            pltpu.VMEM((sides, rows, width), jnp.bfloat16),
            dma((ring,)),
            dma((ring,)),
            dma((ring,)),
            dma((ring,)),
            dma((sides,)),
            dma((sides,)),
            dma((ring,)),
            dma((ring,)),
            dma((ring,)),
            dma((ring,)),
            dma((2,)),
        ],
        compiler_params=pltpu.CompilerParams(
            collective_id=2, has_side_effects=True, vmem_limit_bytes=40 * 1024 * 1024
        ),
        name="merge_targets",
    )(mixed, stats, weights, mine, live)


def project_kernel(share, tokens, gain, w_ref, q_out, kv_out):
    rows = tokens.shape[0]
    part = rows // share
    heads = w_ref.shape[2] // HD
    normed = norm_rows(tokens[...].astype(jnp.float32), gain[...]).astype(jnp.bfloat16)
    scaling = jnp.bfloat16(HD ** (-0.5))
    queries = (
        lax.dot_general(
            w_ref[0], normed, (((0,), (1,)), ((), ())), preferred_element_type=jnp.float32
        ).astype(jnp.bfloat16)
        * scaling
    )
    keys = jnp.dot(normed, w_ref[1], preferred_element_type=jnp.float32).astype(jnp.bfloat16)
    values = jnp.dot(normed, w_ref[2], preferred_element_type=jnp.float32).astype(jnp.bfloat16)
    for h in range(heads):
        cut = slice(h * HD, (h + 1) * HD)
        both = jnp.concatenate([keys[:, cut], values[:, cut]], axis=1)
        for s in range(share):
            at = slice(s * part, (s + 1) * part)
            q_out[h * share + s] = queries[cut, at]
            kv_out[h * share + s] = both[at, :]


def project_heads(share, tokens, gain, weights):
    rows = tokens.shape[0]
    heads = weights.shape[2] // HD
    part = rows // share
    vmem = pl.BlockSpec(memory_space=pltpu.VMEM)
    return pl.pallas_call(
        functools.partial(project_kernel, share),
        out_shape=(
            jax.ShapeDtypeStruct((heads * share, HD, part), jnp.bfloat16),
            jax.ShapeDtypeStruct((heads * share, part, 2 * HD), jnp.bfloat16),
        ),
        in_specs=[vmem, vmem, vmem],
        out_specs=(vmem, vmem),
        compiler_params=pltpu.CompilerParams(vmem_limit_bytes=40 * 1024 * 1024),
        name="project_heads",
    )(tokens, gain[None, :], weights)


def attend_kernel(lengths, q_ref, kv_ref, o_ref, keys, values, flipped, count):
    blocks, span, lanes = kv_ref.shape
    tile = span
    queries = q_ref.shape[1]
    group = math.gcd(queries, 256)
    ones_rows = flipped.shape[1] - HD
    lane = lax.broadcasted_iota(jnp.int32, (span, lanes), 1)
    row = lax.broadcasted_iota(jnp.int32, (span, lanes), 0)

    @pl.when(pl.program_id(0) == 0)
    def pack():
        def place(j, start):
            block = kv_ref[j]
            dead = jnp.where(row < lengths[j], 0.0, masked_score).astype(jnp.bfloat16)
            at = pl.ds(pl.multiple_of(start, 16), span)
            keys[at, :] = jnp.where(lane < HD, block, dead)
            values[at, :] = jnp.where(lane < HD, jnp.ones_like(block), block)
            return start + ((lengths[j] + 15) // 16) * 16

        stop = lax.fori_loop(0, blocks, place, 0)
        at = pl.ds(pl.multiple_of(stop, 16), span)
        keys[at, :] = jnp.where(lane < HD, 0.0, masked_score).astype(jnp.bfloat16)
        values[at, :] = jnp.zeros((span, lanes), jnp.bfloat16)
        count[0] = (stop + tile - 1) // tile

        def flip(t, carry):
            at = pl.ds(pl.multiple_of(t * tile, tile), tile)
            flipped[t] = values[at, :].T[HD - ones_rows :, :]
            return carry

        lax.fori_loop(0, count[0], flip, 0)

    spare = lax.broadcasted_iota(jnp.int32, (HD, queries), 0)
    pick = jnp.where(spare == 0, 1.0, 0.0).astype(jnp.bfloat16)
    q_wide = jnp.concatenate([q_ref[...], pick], axis=0)
    cuts = [slice(g, g + group) for g in range(0, queries, group)]

    def step(t, state):
        at = pl.ds(pl.multiple_of(t * tile, tile), tile)
        keys_here = keys[at, :]
        values_here = flipped[t]
        all_scores = [
            jnp.dot(keys_here, q_wide[:, cut], preferred_element_type=jnp.float32) for cut in cuts
        ]
        updated = []
        for scores, (top, mixed) in zip(all_scores, state):
            new_top = jnp.maximum(top, jnp.max(scores, axis=0, keepdims=True))
            weights = jnp.exp(scores - new_top).astype(jnp.bfloat16)
            part = jnp.dot(values_here, weights, preferred_element_type=jnp.float32)
            updated.append((new_top, mixed * jnp.exp(top - new_top) + part))
        return tuple(updated)

    start = tuple(
        (
            jnp.full((1, group), masked_score, jnp.float32),
            jnp.zeros((ones_rows + HD, group), jnp.float32),
        )
        for cut in cuts
    )
    ends = lax.fori_loop(0, count[0], step, start)
    for cut, (top, mixed) in zip(cuts, ends):
        o_ref[:, cut] = (mixed[ones_rows:, :] / mixed[0:1, :]).astype(jnp.bfloat16)


def attend(q_all, kv_all, pad_lengths):
    blocks, span, lanes = kv_all.shape
    total = q_all.shape[1]
    width = math.gcd(total, 2048)
    return pl.pallas_call(
        attend_kernel,
        out_shape=jax.ShapeDtypeStruct((HD, total), jnp.bfloat16),
        grid_spec=pltpu.PrefetchScalarGridSpec(
            num_scalar_prefetch=1,
            grid=(total // width,),
            in_specs=[
                pl.BlockSpec((HD, width), lambda i, lengths: (0, i)),
                pl.BlockSpec((blocks, span, lanes), lambda i, lengths: (0, 0, 0)),
            ],
            out_specs=pl.BlockSpec((HD, width), lambda i, lengths: (0, i)),
            scratch_shapes=[
                pltpu.VMEM(((blocks + 1) * span, lanes), jnp.bfloat16),
                pltpu.VMEM(((blocks + 1) * span, lanes), jnp.bfloat16),
                pltpu.VMEM((blocks + 1, HD + 16, span), jnp.bfloat16),
                pltpu.SMEM((1,), jnp.int32),
            ],
        ),
        compiler_params=pltpu.CompilerParams(
            dimension_semantics=("arbitrary",), vmem_limit_bytes=48 * 1024 * 1024
        ),
        name="attend",
    )(pad_lengths, q_all, kv_all)


def local(
    ring,
    sides,
    tokens,
    norm_attn,
    self_qkv,
    self_out,
    norm_ffn,
    ffn_in,
    ffn_out,
    norm_final,
    pad_lengths,
    targets,
    target_lengths,
    norm_cross,
    cross_query,
    cross_kv,
    cross_out,
):
    row_count = tokens.shape[0]
    heads_here = self_qkv.shape[2] // HD
    share = ring // heads_here
    part = row_count // share
    q_send, kv_send = project_heads(share, tokens, norm_attn, self_qkv)
    q_got, kv_got, out_all, cross_q = scatter_heads(
        ring, share, sides, q_send, kv_send, self_out, targets, norm_cross, cross_query
    )
    q_all = q_got.transpose(1, 0, 2).reshape(HD, ring * part)
    mixed_t = attend(q_all, kv_got, pad_lengths)
    back = mixed_t.reshape(HD, ring, part).transpose(1, 0, 2)
    encoded = encoder_block(
        ring,
        share,
        sides,
        back,
        out_all.reshape(-1, out_all.shape[2]),
        tokens,
        norm_ffn,
        norm_final,
        ffn_in,
        ffn_out,
    )
    target_rows = targets.shape[0]
    cross_keys = jnp.dot(encoded, cross_kv[0], preferred_element_type=jnp.float32).astype(
        jnp.bfloat16
    )
    cross_values = jnp.dot(encoded, cross_kv[1], preferred_element_type=jnp.float32).astype(
        jnp.bfloat16
    )
    my_length = lax.dynamic_slice_in_dim(pad_lengths, lax.axis_index("seq"), 1, 0)
    mixed, stats = cross_attend(my_length, cross_q, cross_keys, cross_values)
    slice_rows = target_rows // ring
    slots = lax.axis_index("seq") * slice_rows + jnp.arange(slice_rows, dtype=jnp.int32)
    owner = slots // TGT_LEN
    limits = jnp.sum(
        jnp.where(
            owner[:, None] == jnp.arange(target_lengths.shape[0])[None, :],
            target_lengths[None, :],
            0,
        ),
        axis=1,
    )
    target_live = slots % TGT_LEN < limits
    mine = lax.dynamic_slice_in_dim(targets, lax.axis_index("seq") * slice_rows, slice_rows, 0)
    live = jnp.broadcast_to(target_live[:, None], mine.shape).astype(jnp.float32)
    decoded = merge_targets(ring, sides, mixed, stats, cross_out, mine, live)
    return (encoded, decoded)


def cross_kernel(length, q_ref, k_ref, v_ref, o_ref, stats):
    i = pl.program_id(0)
    rows = k_ref.shape[0]
    queries = q_ref.shape[0]
    live = lax.broadcasted_iota(jnp.int32, (queries, rows), 1) < length[0]
    lane = lax.broadcasted_iota(jnp.int32, (rows, 2 * HD), 1)
    out_lane = lax.broadcasted_iota(jnp.int32, (queries, 2 * HD), 1)
    ones = jnp.ones((rows, 2 * HD), jnp.bfloat16)

    @pl.when(i == 0)
    def clear():
        stats[...] = jnp.where(out_lane < HD, 0.0, 1.0)

    pieces = []
    for h in range(2):
        own = lane < HD if h == 0 else lane >= HD
        keys = jnp.where(own, k_ref[...], jnp.zeros_like(ones))
        values = jnp.where(own, v_ref[...], ones)
        scores = lax.dot_general(
            q_ref[...], keys, (((1,), (1,)), ((), ())), preferred_element_type=jnp.float32
        )
        scores = jnp.where(live, scores, masked_score)
        top = jnp.max(scores, axis=1, keepdims=True)
        weights = jnp.exp(scores - top).astype(jnp.bfloat16)
        part = jnp.dot(weights, values, preferred_element_type=jnp.float32)
        total = part[:, 2 * HD - 1 :] if h == 0 else part[:, :1]
        stats[...] = jnp.where(
            out_lane == 2 * i + h,
            top,
            jnp.where(out_lane == HD + 2 * i + h, total, stats[...]),
        )
        pieces.append(part)
    o_ref[...] = jnp.where(out_lane < HD, pieces[0], pieces[1]).astype(jnp.bfloat16)


def cross_attend(my_length, q_all, keys, values):
    rows, width = keys.shape
    queries = q_all.shape[0]
    return pl.pallas_call(
        cross_kernel,
        out_shape=(
            jax.ShapeDtypeStruct((queries, width), jnp.bfloat16),
            jax.ShapeDtypeStruct((queries, 2 * HD), jnp.float32),
        ),
        grid_spec=pltpu.PrefetchScalarGridSpec(
            num_scalar_prefetch=1,
            grid=(width // (2 * HD),),
            in_specs=[
                pl.BlockSpec((queries, 2 * HD), lambda i, n: (0, i)),
                pl.BlockSpec((rows, 2 * HD), lambda i, n: (0, i)),
                pl.BlockSpec((rows, 2 * HD), lambda i, n: (0, i)),
            ],
            out_specs=(
                pl.BlockSpec((queries, 2 * HD), lambda i, n: (0, i)),
                pl.BlockSpec((queries, 2 * HD), lambda i, n: (0, 0)),
            ),
        ),
        compiler_params=pltpu.CompilerParams(
            dimension_semantics=("arbitrary",), vmem_limit_bytes=32 * 1024 * 1024
        ),
        name="cross_attend",
    )(my_length, q_all, keys, values)


def solution(mesh):
    ring = mesh.shape["seq"]
    sides = mesh.shape["head"]
    placed = (
        P("seq", None),
        P(),
        P(None, None, "head"),
        P("head", None),
        P(),
        P(None, None, "head"),
        P("head", None),
        P(),
        P(),
        P(),
        P(),
        P(),
        P(None, "head"),
        P(None, None, "head"),
        P("head", None),
    )
    return jax.shard_map(
        functools.partial(local, ring, sides),
        mesh=mesh,
        in_specs=placed,
        out_specs=(P("seq", None), P()),
        check_vma=False,
    )
```

```python
import functools
import math

import jax
import jax.numpy as jnp
from jax import lax
from jax.experimental import pallas as pl
from jax.experimental.pallas import tpu as pltpu
from jax.sharding import PartitionSpec as P

HD = 64
TOK_DEV = 512
TGT_LEN = 128

epsilon = 1e-06
masked_score = -1e30
MESH = pl.DeviceIdType.MESH


def greet_all(ring, sides):
    me = lax.axis_index("seq")
    here = lax.axis_index("head")
    barrier = pltpu.get_barrier_semaphore()

    def greet(i, carry):
        pl.semaphore_signal(
            barrier, inc=1, device_id={"seq": lax.rem(me + i, ring)}, device_id_type=MESH
        )
        return carry

    lax.fori_loop(1, ring, greet, 0)
    for k in range(1, sides):
        pl.semaphore_signal(
            barrier, inc=1, device_id={"head": lax.rem(here + k, sides)}, device_id_type=MESH
        )
    pl.semaphore_wait(barrier, ring - 1 + sides - 1)


def side_copy(sides, k, source, target, send_sem, recv_sem):
    here = lax.axis_index("head")
    return pltpu.make_async_remote_copy(
        src_ref=source,
        dst_ref=target,
        send_sem=send_sem,
        recv_sem=recv_sem,
        device_id={"head": lax.rem(here + k, sides)},
        device_id_type=MESH,
    )


def scatter_kernel(
    ring, share, sides, q_in, kv_in, w_in, targets, g_cross, w_cross,
    q_out, kv_out, w_out, cross_q, qs, qr, ks, kr, fs, fr, ls, ws, wr,
):
    me = lax.axis_index("seq")
    here = lax.axis_index("head")
    part = kv_in.shape[1]
    mine = pl.ds(pl.multiple_of(lax.rem(me, share) * part, part), part)
    own_q = pltpu.make_async_copy(q_in.at[me], q_out.at[me], ls.at[0])
    own_kv = pltpu.make_async_copy(kv_in.at[me], kv_out.at[me, mine], ls.at[1])
    own_q.start()
    own_kv.start()
    own_w = pltpu.make_async_copy(w_in, w_out.at[here], ls.at[2])
    own_w.start()
    greet_all(ring, sides)

    def q_copy(i):
        to = lax.rem(me + i, ring)
        return pltpu.make_async_remote_copy(
            src_ref=q_in.at[to],
            dst_ref=q_out.at[me],
            send_sem=qs.at[i],
            recv_sem=qr.at[i],
            device_id={"seq": to},
            device_id_type=MESH,
        )

    def kv_copy(i):
        to = lax.rem(me + i, ring)
        rows = pl.ds(pl.multiple_of(lax.rem(to, share) * part, part), part)
        return pltpu.make_async_remote_copy(
            src_ref=kv_in.at[to],
            dst_ref=kv_out.at[me, rows],
            send_sem=ks.at[i],
            recv_sem=kr.at[i],
            device_id={"seq": to},
            device_id_type=MESH,
        )

    def forward(i, k):
        origin = lax.rem(me - i + ring, ring)
        slot = lax.rem(me, share)
        to = me - slot + lax.rem(slot + k, share)
        block = kv_out.at[origin, mine]
        return pltpu.make_async_remote_copy(
            src_ref=block,
            dst_ref=block,
            send_sem=fs.at[i, k],
            recv_sem=fr.at[i, k],
            device_id={"seq": to},
            device_id_type=MESH,
        )

    def arrived(i, k):
        slot = lax.rem(me, share)
        giver = me - slot + lax.rem(slot - k + share, share)
        origin = lax.rem(giver - i + ring, ring)
        rows = pl.ds(pl.multiple_of(lax.rem(giver, share) * part, part), part)
        block = kv_out.at[origin, rows]
        return pltpu.make_async_remote_copy(
            src_ref=block,
            dst_ref=block,
            send_sem=fs.at[i, k],
            recv_sem=fr.at[i, k],
            device_id={"seq": giver},
            device_id_type=MESH,
        )

    def send(i, carry):
        kv_copy(i).start()
        q_copy(i).start()
        return carry

    lax.fori_loop(1, ring, send, 0)
    for k in range(1, sides):
        side_copy(sides, k, w_in, w_out.at[here], ws.at[k], wr.at[k]).start()
    own_kv.wait()
    cross_normed = norm_rows(targets[...].astype(jnp.float32), g_cross[...]).astype(jnp.bfloat16)
    cross_q[...] = jnp.dot(
        cross_normed, w_cross[...], preferred_element_type=jnp.float32
    ).astype(jnp.bfloat16) * jnp.bfloat16(HD ** (-0.5))
    for k in range(1, share):
        forward(0, k).start()

    def relay(i, carry):
        pltpu.make_async_remote_copy(
            src_ref=kv_in.at[0],
            dst_ref=kv_out.at[lax.rem(me - i + ring, ring), mine],
            send_sem=ks.at[i],
            recv_sem=kr.at[i],
            device_id={"seq": lax.rem(me + i, ring)},
            device_id_type=MESH,
        ).wait_recv()
        for k in range(1, share):
            forward(i, k).start()
        return carry

    lax.fori_loop(1, ring, relay, 0)

    def finish(i, carry):
        pltpu.make_async_remote_copy(
            src_ref=q_in.at[0],
            dst_ref=q_out.at[lax.rem(me - i + ring, ring)],
            send_sem=qs.at[i],
            recv_sem=qr.at[i],
            device_id={"seq": lax.rem(me + i, ring)},
            device_id_type=MESH,
        ).wait_recv()
        q_copy(i).wait_send()
        kv_copy(i).wait_send()
        return carry

    lax.fori_loop(1, ring, finish, 0)

    def drain(i, carry):
        for k in range(1, share):
            arrived(i, k).wait_recv()
            forward(i, k).wait_send()
        return carry

    lax.fori_loop(0, ring, drain, 0)
    for k in range(1, sides):
        origin = lax.rem(here - k + sides, sides)
        side_copy(sides, k, w_in, w_out.at[origin], ws.at[k], wr.at[k]).wait()
    own_q.wait()
    own_w.wait()


def scatter_heads(ring, share, sides, q_send, kv_send, weights, targets, g_cross, w_cross):
    part = kv_send.shape[1]
    return pl.pallas_call(
        functools.partial(scatter_kernel, ring, share, sides),
        out_shape=(
            jax.ShapeDtypeStruct(q_send.shape, q_send.dtype),
            jax.ShapeDtypeStruct((ring, part * share, 2 * HD), kv_send.dtype),
            jax.ShapeDtypeStruct((sides,) + weights.shape, weights.dtype),
            jax.ShapeDtypeStruct((targets.shape[0], w_cross.shape[1]), jnp.bfloat16),
        ),
        in_specs=[pl.BlockSpec(memory_space=pltpu.VMEM)] * 6,
        out_specs=(pl.BlockSpec(memory_space=pltpu.VMEM),) * 4,
        scratch_shapes=[
            pltpu.SemaphoreType.DMA((ring,)),
            pltpu.SemaphoreType.DMA((ring,)),
            pltpu.SemaphoreType.DMA((ring,)),
            pltpu.SemaphoreType.DMA((ring,)),
            pltpu.SemaphoreType.DMA((ring, share)),
            pltpu.SemaphoreType.DMA((ring, share)),
            pltpu.SemaphoreType.DMA((3,)),
            pltpu.SemaphoreType.DMA((sides,)),
            pltpu.SemaphoreType.DMA((sides,)),
        ],
        compiler_params=pltpu.CompilerParams(
            collective_id=0, has_side_effects=True, vmem_limit_bytes=40 * 1024 * 1024
        ),
        name="scatter_heads",
    )(q_send, kv_send, weights, targets, g_cross[None, :], w_cross)


def norm_rows(values, gain):
    scale = lax.rsqrt(jnp.mean(values * values, axis=-1, keepdims=True) + epsilon)
    return values * scale * gain


def block_kernel(
    ring, share, sides, x_in, w_out, tokens, g_ffn, g_final, up_hbm, down_hbm,
    kv_hbm, cross_q, bias,
    encoded, mixed, stats,
    context, hidden, normed, parts, up, down, w_kv, cross_k, cross_v,
    ss, rs, fs, fr, ps, pr, ls,
):
    me = lax.axis_index("seq")
    here = lax.axis_index("head")
    heads = ring // share
    rows, width = tokens.shape
    up_load = pltpu.make_async_copy(up_hbm, up, ls.at[0])
    down_load = pltpu.make_async_copy(down_hbm, down, ls.at[1])
    kv_load = pltpu.make_async_copy(kv_hbm, w_kv, ls.at[3])
    up_load.start()
    down_load.start()
    kv_load.start()

    def place(side, origin):
        return context.at[lax.rem(origin, share), side * heads + lax.div(origin, share)]

    own = pltpu.make_async_copy(x_in.at[me], place(here, me), ls.at[2])
    own.start()
    greet_all(ring, sides)

    def outgoing(i):
        to = lax.rem(me + i, ring)
        return pltpu.make_async_remote_copy(
            src_ref=x_in.at[to],
            dst_ref=place(here, me),
            send_sem=ss.at[i],
            recv_sem=rs.at[i],
            device_id={"seq": to},
            device_id_type=MESH,
        )

    def relay(i, k):
        block = place(here, lax.rem(me - i + ring, ring))
        return side_copy(sides, k, block, block, fs.at[i, k], fr.at[i, k])

    def send(i, carry):
        outgoing(i).start()
        return carry

    lax.fori_loop(1, ring, send, 0)
    own.wait()
    for k in range(1, sides):
        relay(0, k).start()

    def pass_on(i, carry):
        pltpu.make_async_remote_copy(
            src_ref=x_in.at[0],
            dst_ref=place(here, lax.rem(me - i + ring, ring)),
            send_sem=ss.at[i],
            recv_sem=rs.at[i],
            device_id={"seq": lax.rem(me + i, ring)},
            device_id_type=MESH,
        ).wait_recv()
        for k in range(1, sides):
            relay(i, k).start()
        return carry

    lax.fori_loop(1, ring, pass_on, 0)

    def sent(i, carry):
        outgoing(i).wait_send()
        return carry

    lax.fori_loop(1, ring, sent, 0)

    def drain(i, carry):
        for k in range(1, sides):
            relay(i, k).wait_send()
            origin = lax.rem(here - k + sides, sides)
            block = place(origin, lax.rem(me - i + ring, ring))
            side_copy(sides, k, block, block, fs.at[i, k], fr.at[i, k]).wait_recv()
        return carry

    lax.fori_loop(0, ring, drain, 0)
    part = rows // share

    def project(c, carry):
        at = pl.ds(pl.multiple_of(c * part, part), part)
        flat = context[c].reshape(sides * heads * HD, part)
        total = tokens[at, :].astype(jnp.float32) + lax.dot_general(
            flat, w_out[...], (((0,), (0,)), ((), ())), preferred_element_type=jnp.float32
        )
        hidden[at, :] = total
        normed[at, :] = norm_rows(total, g_ffn[...]).astype(jnp.bfloat16)
        return carry

    lax.fori_loop(0, share, project, 0)
    up_load.wait()
    down_load.wait()
    chunk = math.gcd(rows, 128)
    chunks = rows // chunk

    def span(c):
        return pl.ds(pl.multiple_of(c * chunk, chunk), chunk)

    def swap(c, k, side):
        return side_copy(
            sides, k, parts.at[side, span(c)], parts.at[side, span(c)], ps.at[c, k], pr.at[c, k]
        )

    def feed(c, carry):
        x = normed[span(c), :]
        gate = jnp.dot(x, up[0], preferred_element_type=jnp.float32)
        lift = jnp.dot(x, up[1], preferred_element_type=jnp.float32)
        active = (jax.nn.gelu(gate, approximate=True) * lift).astype(jnp.bfloat16)
        parts[here, span(c), :] = jnp.dot(
            active, down[...], preferred_element_type=jnp.float32
        ).astype(jnp.bfloat16)
        for k in range(1, sides):
            swap(c, k, here).start()
        return carry

    lax.fori_loop(0, chunks, feed, 0)
    kv_load.wait()

    def close(c, carry):
        for k in range(1, sides):
            swap(c, k, here).wait_send()
            swap(c, k, lax.rem(here - k + sides, sides)).wait_recv()
        total = hidden[span(c), :]
        for side in range(sides):
            total = total + parts[side, span(c), :].astype(jnp.float32)
        done = norm_rows(total, g_final[...]).astype(jnp.bfloat16)
        encoded[span(c), :] = done
        cross_k[span(c), :] = jnp.dot(
            done, w_kv[0], preferred_element_type=jnp.float32
        ).astype(jnp.bfloat16)
        cross_v[span(c), :] = jnp.dot(
            done, w_kv[1], preferred_element_type=jnp.float32
        ).astype(jnp.bfloat16)
        return carry

    lax.fori_loop(0, chunks, close, 0)
    targets = cross_q.shape[0]
    lane = lax.broadcasted_iota(jnp.int32, (rows, 2 * HD), 1)
    out_lane = lax.broadcasted_iota(jnp.int32, (targets, 2 * HD), 1)
    ones = jnp.ones((rows, 2 * HD), jnp.bfloat16)
    stats[...] = jnp.where(out_lane < HD, 0.0, 1.0)

    def cross_pair(i, carry):
        cut = pl.ds(pl.multiple_of(i * 2 * HD, 2 * HD), 2 * HD)
        q_here = cross_q[:, cut]
        k_here = cross_k[:, cut]
        v_here = cross_v[:, cut]
        pieces = []
        seen = stats[...]
        for h in range(2):
            own = lane < HD if h == 0 else lane >= HD
            keys = jnp.where(own, k_here, jnp.zeros_like(ones))
            values = jnp.where(own, v_here, ones)
            scores = bias[...] + lax.dot_general(
                q_here, keys, (((1,), (1,)), ((), ())), preferred_element_type=jnp.float32
            )
            top = jnp.max(scores, axis=1, keepdims=True)
            weights = jnp.exp(scores - top).astype(jnp.bfloat16)
            piece = jnp.dot(weights, values, preferred_element_type=jnp.float32)
            total = piece[:, 2 * HD - 1 :] if h == 0 else piece[:, :1]
            seen = jnp.where(
                out_lane == 2 * i + h, top, jnp.where(out_lane == HD + 2 * i + h, total, seen)
            )
            pieces.append(piece)
        stats[...] = seen
        mixed[:, cut] = jnp.where(out_lane < HD, pieces[0], pieces[1]).astype(jnp.bfloat16)
        return carry

    lax.fori_loop(0, heads // 2, cross_pair, 0)


def encoder_block(
    ring, share, sides, back, w_out, tokens, g_ffn, g_final, ffn_in, ffn_out, w_kv, cross_q, bias
):
    rows, width = tokens.shape
    chunks = rows // math.gcd(rows, 128)
    vmem = pl.BlockSpec(memory_space=pltpu.VMEM)
    hbm = pl.BlockSpec(memory_space=pl.ANY)
    return pl.pallas_call(
        functools.partial(block_kernel, ring, share, sides),
        out_shape=(
            jax.ShapeDtypeStruct((rows, width), jnp.bfloat16),
            jax.ShapeDtypeStruct(cross_q.shape, jnp.bfloat16),
            jax.ShapeDtypeStruct((cross_q.shape[0], 2 * HD), jnp.float32),
        ),
        in_specs=[vmem, vmem, vmem, vmem, vmem, hbm, hbm, hbm, vmem, vmem],
        out_specs=(vmem, vmem, vmem),
        scratch_shapes=[
            pltpu.VMEM((share, sides * (ring // share), HD, rows // share), jnp.bfloat16),
            pltpu.VMEM((rows, width), jnp.float32),
            pltpu.VMEM((rows, width), jnp.bfloat16),
            pltpu.VMEM((sides, rows, width), jnp.bfloat16),
            pltpu.VMEM(ffn_in.shape, jnp.bfloat16),
            pltpu.VMEM(ffn_out.shape, jnp.bfloat16),
            pltpu.VMEM(w_kv.shape, jnp.bfloat16),
            pltpu.VMEM((rows, w_kv.shape[2]), jnp.bfloat16),
            pltpu.VMEM((rows, w_kv.shape[2]), jnp.bfloat16),
            pltpu.SemaphoreType.DMA((ring,)),
            pltpu.SemaphoreType.DMA((ring,)),
            pltpu.SemaphoreType.DMA((ring, sides)),
            pltpu.SemaphoreType.DMA((ring, sides)),
            pltpu.SemaphoreType.DMA((chunks, sides)),
            pltpu.SemaphoreType.DMA((chunks, sides)),
            pltpu.SemaphoreType.DMA((4,)),
        ],
        compiler_params=pltpu.CompilerParams(
            collective_id=1, has_side_effects=True, vmem_limit_bytes=50 * 1024 * 1024
        ),
        name="encoder_block",
    )(
        back, w_out, tokens, g_ffn[None, :], g_final[None, :], ffn_in, ffn_out, w_kv, cross_q, bias
    )


def merge_kernel(
    ring, sides, mixed, stats, w_ref, mine, live, decoded,
    got, got_stats, parts, ms, mr, ts, tr, ps, pr, ds, dr, fs, fr, ls,
):
    me = lax.axis_index("seq")
    here = lax.axis_index("head")
    rows, width = mine.shape
    mate = me + 1 - 2 * lax.rem(me, 2)

    def slab(owner):
        return pl.ds(pl.multiple_of(owner * rows, rows), rows)

    own_mixed = pltpu.make_async_copy(mixed.at[slab(me)], got.at[me], ls.at[0])
    own_stats = pltpu.make_async_copy(stats.at[slab(me)], got_stats.at[me], ls.at[1])
    own_mixed.start()
    own_stats.start()
    greet_all(ring, sides)

    def copies(i, origin):
        to = lax.rem(me + i, ring)
        return (
            pltpu.make_async_remote_copy(
                src_ref=mixed.at[slab(to)],
                dst_ref=got.at[origin],
                send_sem=ms.at[i],
                recv_sem=mr.at[i],
                device_id={"seq": to},
                device_id_type=MESH,
            ),
            pltpu.make_async_remote_copy(
                src_ref=stats.at[slab(to)],
                dst_ref=got_stats.at[origin],
                send_sem=ts.at[i],
                recv_sem=tr.at[i],
                device_id={"seq": to},
                device_id_type=MESH,
            ),
        )

    def send(i, carry):
        for copy in copies(i, me):
            copy.start()
        return carry

    lax.fori_loop(1, ring, send, 0)

    def collect(i, carry):
        for copy in copies(i, lax.rem(me - i + ring, ring)):
            copy.wait()
        return carry

    lax.fori_loop(1, ring, collect, 0)
    own_mixed.wait()
    own_stats.wait()
    heads = w_ref.shape[0] // HD
    seen = got_stats[...]
    best = jnp.max(seen, axis=0, keepdims=True)
    grow = jnp.exp(seen - best)
    sums = pltpu.roll(seen.reshape(ring * rows, 2 * HD), HD, 1).reshape(ring, rows, 2 * HD)
    weight_sum = jnp.sum(grow * sums, axis=0, keepdims=True)
    factor = (grow / weight_sum).reshape(ring * rows, 2 * HD)
    lane = lax.broadcasted_iota(jnp.int32, (2 * HD, heads * HD), 1)
    row = lax.broadcasted_iota(jnp.int32, (2 * HD, heads * HD), 0)
    spread = jnp.where((lane >= row * HD) & (lane < row * HD + HD), 1.0, 0.0)
    factor = jnp.where(
        lax.broadcasted_iota(jnp.int32, factor.shape, 1) < heads, factor, 0.0
    )
    wide = jnp.dot(
        factor, spread, precision=lax.Precision.HIGHEST, preferred_element_type=jnp.float32
    ).reshape(ring, rows, heads * HD)
    context = jnp.sum(got[...].astype(jnp.float32) * wide, axis=0).astype(jnp.bfloat16)
    parts[here] = jnp.dot(context, w_ref[...], preferred_element_type=jnp.float32).astype(
        jnp.bfloat16
    )

    def swap(k, side):
        return side_copy(sides, k, parts.at[side], parts.at[side], ps.at[k], pr.at[k])

    for k in range(1, sides):
        swap(k, here).start()
    for k in range(1, sides):
        swap(k, here).wait_send()
        swap(k, lax.rem(here - k + sides, sides)).wait_recv()
    total = parts[0].astype(jnp.float32)
    for side in range(1, sides):
        total = total + parts[side].astype(jnp.float32)
    decoded[slab(me), :] = (
        mine[...].astype(jnp.float32) + jnp.where(live[...] > 0.0, total, 0.0)
    ).astype(jnp.bfloat16)

    def spread_out(j, owner):
        block = decoded.at[slab(owner)]
        return pltpu.make_async_remote_copy(
            src_ref=block,
            dst_ref=block,
            send_sem=ds.at[j],
            recv_sem=dr.at[j],
            device_id={"seq": lax.rem(me + 2 * j, ring)},
            device_id_type=MESH,
        )

    def hand_over(j, owner):
        block = decoded.at[slab(owner)]
        return pltpu.make_async_remote_copy(
            src_ref=block,
            dst_ref=block,
            send_sem=fs.at[j],
            recv_sem=fr.at[j],
            device_id={"seq": mate},
            device_id_type=MESH,
        )

    def share_out(j, carry):
        spread_out(j, me).start()
        return carry

    lax.fori_loop(1, ring // 2, share_out, 0)
    hand_over(0, me).start()

    def pass_on(j, carry):
        owner = lax.rem(me - 2 * j + ring, ring)
        spread_out(j, owner).wait_recv()
        hand_over(j, owner).start()
        return carry

    lax.fori_loop(1, ring // 2, pass_on, 0)

    def finish(j, carry):
        spread_out(j, me).wait_send()
        return carry

    lax.fori_loop(1, ring // 2, finish, 0)

    def drain(j, carry):
        hand_over(j, lax.rem(me - 2 * j + ring, ring)).wait_send()
        hand_over(j, lax.rem(mate - 2 * j + ring, ring)).wait_recv()
        return carry

    lax.fori_loop(0, ring // 2, drain, 0)


def merge_targets(ring, sides, mixed, stats, weights, mine, live):
    rows, width = mine.shape
    vmem = pl.BlockSpec(memory_space=pltpu.VMEM)
    dma = pltpu.SemaphoreType.DMA
    return pl.pallas_call(
        functools.partial(merge_kernel, ring, sides),
        out_shape=jax.ShapeDtypeStruct((rows * ring, width), jnp.bfloat16),
        in_specs=[vmem] * 5,
        out_specs=vmem,
        scratch_shapes=[
            pltpu.VMEM((ring, rows, mixed.shape[1]), jnp.bfloat16),
            pltpu.VMEM((ring, rows, stats.shape[1]), jnp.float32),
            pltpu.VMEM((sides, rows, width), jnp.bfloat16),
            dma((ring,)),
            dma((ring,)),
            dma((ring,)),
            dma((ring,)),
            dma((sides,)),
            dma((sides,)),
            dma((ring,)),
            dma((ring,)),
            dma((ring,)),
            dma((ring,)),
            dma((2,)),
        ],
        compiler_params=pltpu.CompilerParams(
            collective_id=2, has_side_effects=True, vmem_limit_bytes=40 * 1024 * 1024
        ),
        name="merge_targets",
    )(mixed, stats, weights, mine, live)


def project_kernel(share, tokens, gain, w_ref, q_out, kv_out):
    rows = tokens.shape[0]
    part = rows // share
    heads = w_ref.shape[2] // HD
    normed = norm_rows(tokens[...].astype(jnp.float32), gain[...]).astype(jnp.bfloat16)
    scaling = jnp.bfloat16(HD ** (-0.5))
    queries = (
        lax.dot_general(
            w_ref[0], normed, (((0,), (1,)), ((), ())), preferred_element_type=jnp.float32
        ).astype(jnp.bfloat16)
        * scaling
    )
    keys = jnp.dot(normed, w_ref[1], preferred_element_type=jnp.float32).astype(jnp.bfloat16)
    values = jnp.dot(normed, w_ref[2], preferred_element_type=jnp.float32).astype(jnp.bfloat16)
    for h in range(heads):
        cut = slice(h * HD, (h + 1) * HD)
        both = jnp.concatenate([keys[:, cut], values[:, cut]], axis=1)
        for s in range(share):
            at = slice(s * part, (s + 1) * part)
            q_out[h * share + s] = queries[cut, at]
            kv_out[h * share + s] = both[at, :]


def project_heads(share, tokens, gain, weights):
    rows = tokens.shape[0]
    heads = weights.shape[2] // HD
    part = rows // share
    vmem = pl.BlockSpec(memory_space=pltpu.VMEM)
    return pl.pallas_call(
        functools.partial(project_kernel, share),
        out_shape=(
            jax.ShapeDtypeStruct((heads * share, HD, part), jnp.bfloat16),
            jax.ShapeDtypeStruct((heads * share, part, 2 * HD), jnp.bfloat16),
        ),
        in_specs=[vmem, vmem, vmem],
        out_specs=(vmem, vmem),
        compiler_params=pltpu.CompilerParams(vmem_limit_bytes=40 * 1024 * 1024),
        name="project_heads",
    )(tokens, gain[None, :], weights)


def attend_kernel(lengths, q_ref, kv_ref, o_ref, keys, values, flipped, count):
    blocks, span, lanes = kv_ref.shape
    tile = span
    queries = q_ref.shape[1]
    group = math.gcd(queries, 256)
    ones_rows = flipped.shape[1] - HD
    lane = lax.broadcasted_iota(jnp.int32, (span, lanes), 1)
    row = lax.broadcasted_iota(jnp.int32, (span, lanes), 0)

    @pl.when(pl.program_id(0) == 0)
    def pack():
        def place(j, start):
            block = kv_ref[j]
            dead = jnp.where(row < lengths[j], 0.0, masked_score).astype(jnp.bfloat16)
            at = pl.ds(pl.multiple_of(start, 16), span)
            keys[at, :] = jnp.where(lane < HD, block, dead)
            values[at, :] = jnp.where(lane < HD, jnp.ones_like(block), block)
            return start + ((lengths[j] + 15) // 16) * 16

        stop = lax.fori_loop(0, blocks, place, 0)
        at = pl.ds(pl.multiple_of(stop, 16), span)
        keys[at, :] = jnp.where(lane < HD, 0.0, masked_score).astype(jnp.bfloat16)
        values[at, :] = jnp.zeros((span, lanes), jnp.bfloat16)
        count[0] = (stop + tile - 1) // tile

        def flip(t, carry):
            at = pl.ds(pl.multiple_of(t * tile, tile), tile)
            flipped[t] = values[at, :].T[HD - ones_rows :, :]
            return carry

        lax.fori_loop(0, count[0], flip, 0)

    spare = lax.broadcasted_iota(jnp.int32, (HD, queries), 0)
    pick = jnp.where(spare == 0, 1.0, 0.0).astype(jnp.bfloat16)
    q_wide = jnp.concatenate([q_ref[...], pick], axis=0)
    cuts = [slice(g, g + group) for g in range(0, queries, group)]

    def step(t, state):
        at = pl.ds(pl.multiple_of(t * tile, tile), tile)
        keys_here = keys[at, :]
        values_here = flipped[t]
        all_scores = [
            jnp.dot(keys_here, q_wide[:, cut], preferred_element_type=jnp.float32) for cut in cuts
        ]
        updated = []
        for scores, (top, mixed) in zip(all_scores, state):
            new_top = jnp.maximum(top, jnp.max(scores, axis=0, keepdims=True))
            weights = jnp.exp(scores - new_top).astype(jnp.bfloat16)
            part = jnp.dot(values_here, weights, preferred_element_type=jnp.float32)
            updated.append((new_top, mixed * jnp.exp(top - new_top) + part))
        return tuple(updated)

    start = tuple(
        (
            jnp.full((1, group), masked_score, jnp.float32),
            jnp.zeros((ones_rows + HD, group), jnp.float32),
        )
        for cut in cuts
    )
    ends = lax.fori_loop(0, count[0], step, start)
    for cut, (top, mixed) in zip(cuts, ends):
        o_ref[:, cut] = (mixed[ones_rows:, :] / mixed[0:1, :]).astype(jnp.bfloat16)


def attend(q_all, kv_all, pad_lengths):
    blocks, span, lanes = kv_all.shape
    total = q_all.shape[1]
    width = math.gcd(total, 2048)
    return pl.pallas_call(
        attend_kernel,
        out_shape=jax.ShapeDtypeStruct((HD, total), jnp.bfloat16),
        grid_spec=pltpu.PrefetchScalarGridSpec(
            num_scalar_prefetch=1,
            grid=(total // width,),
            in_specs=[
                pl.BlockSpec((HD, width), lambda i, lengths: (0, i)),
                pl.BlockSpec((blocks, span, lanes), lambda i, lengths: (0, 0, 0)),
            ],
            out_specs=pl.BlockSpec((HD, width), lambda i, lengths: (0, i)),
            scratch_shapes=[
                pltpu.VMEM(((blocks + 1) * span, lanes), jnp.bfloat16),
                pltpu.VMEM(((blocks + 1) * span, lanes), jnp.bfloat16),
                pltpu.VMEM((blocks + 1, HD + 16, span), jnp.bfloat16),
                pltpu.SMEM((1,), jnp.int32),
            ],
        ),
        compiler_params=pltpu.CompilerParams(
            dimension_semantics=("arbitrary",), vmem_limit_bytes=48 * 1024 * 1024
        ),
        name="attend",
    )(pad_lengths, q_all, kv_all)


def local(
    ring,
    sides,
    tokens,
    norm_attn,
    self_qkv,
    self_out,
    norm_ffn,
    ffn_in,
    ffn_out,
    norm_final,
    pad_lengths,
    targets,
    target_lengths,
    norm_cross,
    cross_query,
    cross_kv,
    cross_out,
):
    row_count = tokens.shape[0]
    heads_here = self_qkv.shape[2] // HD
    share = ring // heads_here
    part = row_count // share
    q_send, kv_send = project_heads(share, tokens, norm_attn, self_qkv)
    q_got, kv_got, out_all, cross_q = scatter_heads(
        ring, share, sides, q_send, kv_send, self_out, targets, norm_cross, cross_query
    )
    q_all = q_got.transpose(1, 0, 2).reshape(HD, ring * part)
    mixed_t = attend(q_all, kv_got, pad_lengths)
    back = mixed_t.reshape(HD, ring, part).transpose(1, 0, 2)
    my_length = lax.dynamic_slice_in_dim(pad_lengths, lax.axis_index("seq"), 1, 0)
    bias = jnp.where(
        jnp.arange(row_count, dtype=jnp.int32)[None, :] < my_length[0], 0.0, masked_score
    ).astype(jnp.float32)
    encoded, mixed, stats = encoder_block(
        ring,
        share,
        sides,
        back,
        out_all.reshape(-1, out_all.shape[2]),
        tokens,
        norm_ffn,
        norm_final,
        ffn_in,
        ffn_out,
        cross_kv,
        cross_q,
        bias,
    )
    target_rows = targets.shape[0]
    slice_rows = target_rows // ring
    slots = lax.axis_index("seq") * slice_rows + jnp.arange(slice_rows, dtype=jnp.int32)
    owner = slots // TGT_LEN
    limits = jnp.sum(
        jnp.where(
            owner[:, None] == jnp.arange(target_lengths.shape[0])[None, :],
            target_lengths[None, :],
            0,
        ),
        axis=1,
    )
    target_live = slots % TGT_LEN < limits
    mine = lax.dynamic_slice_in_dim(targets, lax.axis_index("seq") * slice_rows, slice_rows, 0)
    live = jnp.broadcast_to(target_live[:, None], mine.shape).astype(jnp.float32)
    decoded = merge_targets(ring, sides, mixed, stats, cross_out, mine, live)
    return (encoded, decoded)


def solution(mesh):
    ring = mesh.shape["seq"]
    sides = mesh.shape["head"]
    placed = (
        P("seq", None),
        P(),
        P(None, None, "head"),
        P("head", None),
        P(),
        P(None, None, "head"),
        P("head", None),
        P(),
        P(),
        P(),
        P(),
        P(),
        P(None, "head"),
        P(None, None, "head"),
        P("head", None),
    )
    return jax.shard_map(
        functools.partial(local, ring, sides),
        mesh=mesh,
        in_specs=placed,
        out_specs=(P("seq", None), P()),
        check_vma=False,
    )
```

```python
import functools
import math

import jax
import jax.numpy as jnp
from jax import lax
from jax.experimental import pallas as pl
from jax.experimental.pallas import tpu as pltpu
from jax.sharding import PartitionSpec as P

HD = 64
TOK_DEV = 512
TGT_LEN = 128

epsilon = 1e-06
masked_score = -1e30
MESH = pl.DeviceIdType.MESH


def greet_all(ring, sides):
    me = lax.axis_index("seq")
    here = lax.axis_index("head")
    barrier = pltpu.get_barrier_semaphore()

    def greet(i, carry):
        pl.semaphore_signal(
            barrier, inc=1, device_id={"seq": lax.rem(me + i, ring)}, device_id_type=MESH
        )
        return carry

    lax.fori_loop(1, ring, greet, 0)
    for k in range(1, sides):
        pl.semaphore_signal(
            barrier, inc=1, device_id={"head": lax.rem(here + k, sides)}, device_id_type=MESH
        )
    pl.semaphore_wait(barrier, ring - 1 + sides - 1)


def side_copy(sides, k, source, target, send_sem, recv_sem):
    here = lax.axis_index("head")
    return pltpu.make_async_remote_copy(
        src_ref=source,
        dst_ref=target,
        send_sem=send_sem,
        recv_sem=recv_sem,
        device_id={"head": lax.rem(here + k, sides)},
        device_id_type=MESH,
    )


def scatter_kernel(
    ring, share, sides, q_in, kv_in, w_in, targets, g_cross, w_cross,
    q_out, kv_out, w_out, cross_q, qs, qr, ks, kr, fs, fr, ls, ws, wr,
):
    me = lax.axis_index("seq")
    here = lax.axis_index("head")
    part = kv_in.shape[1]
    mine = pl.ds(pl.multiple_of(lax.rem(me, share) * part, part), part)
    own_q = pltpu.make_async_copy(q_in.at[me], q_out.at[me], ls.at[0])
    own_kv = pltpu.make_async_copy(kv_in.at[me], kv_out.at[me, mine], ls.at[1])
    own_q.start()
    own_kv.start()
    own_w = pltpu.make_async_copy(w_in, w_out.at[here], ls.at[2])
    own_w.start()
    greet_all(ring, sides)

    def q_copy(i):
        to = lax.rem(me + i, ring)
        return pltpu.make_async_remote_copy(
            src_ref=q_in.at[to],
            dst_ref=q_out.at[me],
            send_sem=qs.at[i],
            recv_sem=qr.at[i],
            device_id={"seq": to},
            device_id_type=MESH,
        )

    def kv_copy(i):
        to = lax.rem(me + i, ring)
        rows = pl.ds(pl.multiple_of(lax.rem(to, share) * part, part), part)
        return pltpu.make_async_remote_copy(
            src_ref=kv_in.at[to],
            dst_ref=kv_out.at[me, rows],
            send_sem=ks.at[i],
            recv_sem=kr.at[i],
            device_id={"seq": to},
            device_id_type=MESH,
        )

    def forward(i, k):
        origin = lax.rem(me - i + ring, ring)
        slot = lax.rem(me, share)
        to = me - slot + lax.rem(slot + k, share)
        block = kv_out.at[origin, mine]
        return pltpu.make_async_remote_copy(
            src_ref=block,
            dst_ref=block,
            send_sem=fs.at[i, k],
            recv_sem=fr.at[i, k],
            device_id={"seq": to},
            device_id_type=MESH,
        )

    def arrived(i, k):
        slot = lax.rem(me, share)
        giver = me - slot + lax.rem(slot - k + share, share)
        origin = lax.rem(giver - i + ring, ring)
        rows = pl.ds(pl.multiple_of(lax.rem(giver, share) * part, part), part)
        block = kv_out.at[origin, rows]
        return pltpu.make_async_remote_copy(
            src_ref=block,
            dst_ref=block,
            send_sem=fs.at[i, k],
            recv_sem=fr.at[i, k],
            device_id={"seq": giver},
            device_id_type=MESH,
        )

    def send(i, carry):
        kv_copy(i).start()
        q_copy(i).start()
        return carry

    lax.fori_loop(1, ring, send, 0)
    for k in range(1, sides):
        side_copy(sides, k, w_in, w_out.at[here], ws.at[k], wr.at[k]).start()
    own_kv.wait()
    cross_normed = norm_rows(targets[...].astype(jnp.float32), g_cross[...]).astype(jnp.bfloat16)
    cross_q[...] = jnp.dot(
        cross_normed, w_cross[...], preferred_element_type=jnp.float32
    ).astype(jnp.bfloat16) * jnp.bfloat16(HD ** (-0.5))
    for k in range(1, share):
        forward(0, k).start()

    def relay(i, carry):
        pltpu.make_async_remote_copy(
            src_ref=kv_in.at[0],
            dst_ref=kv_out.at[lax.rem(me - i + ring, ring), mine],
            send_sem=ks.at[i],
            recv_sem=kr.at[i],
            device_id={"seq": lax.rem(me + i, ring)},
            device_id_type=MESH,
        ).wait_recv()
        for k in range(1, share):
            forward(i, k).start()
        return carry

    lax.fori_loop(1, ring, relay, 0)

    def finish(i, carry):
        pltpu.make_async_remote_copy(
            src_ref=q_in.at[0],
            dst_ref=q_out.at[lax.rem(me - i + ring, ring)],
            send_sem=qs.at[i],
            recv_sem=qr.at[i],
            device_id={"seq": lax.rem(me + i, ring)},
            device_id_type=MESH,
        ).wait_recv()
        q_copy(i).wait_send()
        kv_copy(i).wait_send()
        return carry

    lax.fori_loop(1, ring, finish, 0)

    def drain(i, carry):
        for k in range(1, share):
            arrived(i, k).wait_recv()
            forward(i, k).wait_send()
        return carry

    lax.fori_loop(0, ring, drain, 0)
    for k in range(1, sides):
        origin = lax.rem(here - k + sides, sides)
        side_copy(sides, k, w_in, w_out.at[origin], ws.at[k], wr.at[k]).wait()
    own_q.wait()
    own_w.wait()


def scatter_heads(ring, share, sides, q_send, kv_send, weights, targets, g_cross, w_cross):
    part = kv_send.shape[1]
    return pl.pallas_call(
        functools.partial(scatter_kernel, ring, share, sides),
        out_shape=(
            jax.ShapeDtypeStruct(q_send.shape, q_send.dtype),
            jax.ShapeDtypeStruct((ring, part * share, 2 * HD), kv_send.dtype),
            jax.ShapeDtypeStruct((sides,) + weights.shape, weights.dtype),
            jax.ShapeDtypeStruct((targets.shape[0], w_cross.shape[1]), jnp.bfloat16),
        ),
        in_specs=[pl.BlockSpec(memory_space=pltpu.VMEM)] * 6,
        out_specs=(pl.BlockSpec(memory_space=pltpu.VMEM),) * 4,
        scratch_shapes=[
            pltpu.SemaphoreType.DMA((ring,)),
            pltpu.SemaphoreType.DMA((ring,)),
            pltpu.SemaphoreType.DMA((ring,)),
            pltpu.SemaphoreType.DMA((ring,)),
            pltpu.SemaphoreType.DMA((ring, share)),
            pltpu.SemaphoreType.DMA((ring, share)),
            pltpu.SemaphoreType.DMA((3,)),
            pltpu.SemaphoreType.DMA((sides,)),
            pltpu.SemaphoreType.DMA((sides,)),
        ],
        compiler_params=pltpu.CompilerParams(
            collective_id=0, has_side_effects=True, vmem_limit_bytes=40 * 1024 * 1024
        ),
        name="scatter_heads",
    )(q_send, kv_send, weights, targets, g_cross[None, :], w_cross)


def norm_rows(values, gain):
    scale = lax.rsqrt(jnp.mean(values * values, axis=-1, keepdims=True) + epsilon)
    return values * scale * gain


def block_kernel(
    ring, share, sides, x_in, w_out, tokens, g_ffn, g_final, up_hbm, down_hbm,
    kv_hbm, cross_q, bias, w_cross, mine, live,
    encoded, decoded,
    context, hidden, normed, parts, up, down, w_kv, cross_k, cross_v,
    mixed, stats, ss, rs, fs, fr, ps, pr, ls, *tail
):
    me = lax.axis_index("seq")
    here = lax.axis_index("head")
    heads = ring // share
    rows, width = tokens.shape
    up_load = pltpu.make_async_copy(up_hbm, up, ls.at[0])
    down_load = pltpu.make_async_copy(down_hbm, down, ls.at[1])
    kv_load = pltpu.make_async_copy(kv_hbm, w_kv, ls.at[3])
    up_load.start()
    down_load.start()
    kv_load.start()

    def place(side, origin):
        return context.at[lax.rem(origin, share), side * heads + lax.div(origin, share)]

    own = pltpu.make_async_copy(x_in.at[me], place(here, me), ls.at[2])
    own.start()
    greet_all(ring, sides)

    def outgoing(i):
        to = lax.rem(me + i, ring)
        return pltpu.make_async_remote_copy(
            src_ref=x_in.at[to],
            dst_ref=place(here, me),
            send_sem=ss.at[i],
            recv_sem=rs.at[i],
            device_id={"seq": to},
            device_id_type=MESH,
        )

    def relay(i, k):
        block = place(here, lax.rem(me - i + ring, ring))
        return side_copy(sides, k, block, block, fs.at[i, k], fr.at[i, k])

    def send(i, carry):
        outgoing(i).start()
        return carry

    lax.fori_loop(1, ring, send, 0)
    own.wait()
    for k in range(1, sides):
        relay(0, k).start()

    def pass_on(i, carry):
        pltpu.make_async_remote_copy(
            src_ref=x_in.at[0],
            dst_ref=place(here, lax.rem(me - i + ring, ring)),
            send_sem=ss.at[i],
            recv_sem=rs.at[i],
            device_id={"seq": lax.rem(me + i, ring)},
            device_id_type=MESH,
        ).wait_recv()
        for k in range(1, sides):
            relay(i, k).start()
        return carry

    lax.fori_loop(1, ring, pass_on, 0)

    def sent(i, carry):
        outgoing(i).wait_send()
        return carry

    lax.fori_loop(1, ring, sent, 0)

    def drain(i, carry):
        for k in range(1, sides):
            relay(i, k).wait_send()
            origin = lax.rem(here - k + sides, sides)
            block = place(origin, lax.rem(me - i + ring, ring))
            side_copy(sides, k, block, block, fs.at[i, k], fr.at[i, k]).wait_recv()
        return carry

    lax.fori_loop(0, ring, drain, 0)
    part = rows // share

    def project(c, carry):
        at = pl.ds(pl.multiple_of(c * part, part), part)
        flat = context[c].reshape(sides * heads * HD, part)
        total = tokens[at, :].astype(jnp.float32) + lax.dot_general(
            flat, w_out[...], (((0,), (0,)), ((), ())), preferred_element_type=jnp.float32
        )
        hidden[at, :] = total
        normed[at, :] = norm_rows(total, g_ffn[...]).astype(jnp.bfloat16)
        return carry

    lax.fori_loop(0, share, project, 0)
    up_load.wait()
    down_load.wait()
    chunk = math.gcd(rows, 128)
    chunks = rows // chunk

    def span(c):
        return pl.ds(pl.multiple_of(c * chunk, chunk), chunk)

    def swap(c, k, side):
        return side_copy(
            sides, k, parts.at[side, span(c)], parts.at[side, span(c)], ps.at[c, k], pr.at[c, k]
        )

    def feed(c, carry):
        x = normed[span(c), :]
        gate = jnp.dot(x, up[0], preferred_element_type=jnp.float32)
        lift = jnp.dot(x, up[1], preferred_element_type=jnp.float32)
        active = (jax.nn.gelu(gate, approximate=True) * lift).astype(jnp.bfloat16)
        parts[here, span(c), :] = jnp.dot(
            active, down[...], preferred_element_type=jnp.float32
        ).astype(jnp.bfloat16)
        for k in range(1, sides):
            swap(c, k, here).start()
        return carry

    lax.fori_loop(0, chunks, feed, 0)
    kv_load.wait()

    def close(c, carry):
        for k in range(1, sides):
            swap(c, k, here).wait_send()
            swap(c, k, lax.rem(here - k + sides, sides)).wait_recv()
        total = hidden[span(c), :]
        for side in range(sides):
            total = total + parts[side, span(c), :].astype(jnp.float32)
        done = norm_rows(total, g_final[...]).astype(jnp.bfloat16)
        encoded[span(c), :] = done
        cross_k[span(c), :] = jnp.dot(
            done, w_kv[0], preferred_element_type=jnp.float32
        ).astype(jnp.bfloat16)
        cross_v[span(c), :] = jnp.dot(
            done, w_kv[1], preferred_element_type=jnp.float32
        ).astype(jnp.bfloat16)
        return carry

    lax.fori_loop(0, chunks, close, 0)
    targets = cross_q.shape[0]
    lane = lax.broadcasted_iota(jnp.int32, (rows, 2 * HD), 1)
    out_lane = lax.broadcasted_iota(jnp.int32, (targets, 2 * HD), 1)
    ones = jnp.ones((rows, 2 * HD), jnp.bfloat16)
    stats[...] = jnp.where(out_lane < HD, 0.0, 1.0)

    def cross_pair(i, carry):
        cut = pl.ds(pl.multiple_of(i * 2 * HD, 2 * HD), 2 * HD)
        q_here = cross_q[:, cut]
        k_here = cross_k[:, cut]
        v_here = cross_v[:, cut]
        pieces = []
        seen = stats[...]
        for h in range(2):
            own = lane < HD if h == 0 else lane >= HD
            keys = jnp.where(own, k_here, jnp.zeros_like(ones))
            values = jnp.where(own, v_here, ones)
            scores = bias[...] + lax.dot_general(
                q_here, keys, (((1,), (1,)), ((), ())), preferred_element_type=jnp.float32
            )
            top = jnp.max(scores, axis=1, keepdims=True)
            weights = jnp.exp(scores - top).astype(jnp.bfloat16)
            piece = jnp.dot(weights, values, preferred_element_type=jnp.float32)
            total = piece[:, 2 * HD - 1 :] if h == 0 else piece[:, :1]
            seen = jnp.where(
                out_lane == 2 * i + h, top, jnp.where(out_lane == HD + 2 * i + h, total, seen)
            )
            pieces.append(piece)
        stats[...] = seen
        mixed[:, cut] = jnp.where(out_lane < HD, pieces[0], pieces[1]).astype(jnp.bfloat16)
        return carry

    lax.fori_loop(0, heads // 2, cross_pair, 0)
    merge_tail(ring, sides, mixed, stats, w_cross, mine, live, decoded, *tail)


def encoder_block(
    ring, share, sides, back, w_out, tokens, g_ffn, g_final, ffn_in, ffn_out, w_kv, cross_q, bias,
    w_cross, mine, live,
):
    rows, width = tokens.shape
    chunks = rows // math.gcd(rows, 128)
    vmem = pl.BlockSpec(memory_space=pltpu.VMEM)
    hbm = pl.BlockSpec(memory_space=pl.ANY)
    return pl.pallas_call(
        functools.partial(block_kernel, ring, share, sides),
        out_shape=(
            jax.ShapeDtypeStruct((rows, width), jnp.bfloat16),
            jax.ShapeDtypeStruct((cross_q.shape[0], width), jnp.bfloat16),
        ),
        in_specs=[vmem] * 5 + [hbm] * 3 + [vmem] * 5,
        out_specs=(vmem, vmem),
        scratch_shapes=[
            pltpu.VMEM((share, sides * (ring // share), HD, rows // share), jnp.bfloat16),
            pltpu.VMEM((rows, width), jnp.float32),
            pltpu.VMEM((rows, width), jnp.bfloat16),
            pltpu.VMEM((sides, rows, width), jnp.bfloat16),
            pltpu.VMEM(ffn_in.shape, jnp.bfloat16),
            pltpu.VMEM(ffn_out.shape, jnp.bfloat16),
            pltpu.VMEM(w_kv.shape, jnp.bfloat16),
            pltpu.VMEM((rows, w_kv.shape[2]), jnp.bfloat16),
            pltpu.VMEM((rows, w_kv.shape[2]), jnp.bfloat16),
            pltpu.VMEM(cross_q.shape, jnp.bfloat16),
            pltpu.VMEM((cross_q.shape[0], 2 * HD), jnp.float32),
            pltpu.SemaphoreType.DMA((ring,)),
            pltpu.SemaphoreType.DMA((ring,)),
            pltpu.SemaphoreType.DMA((ring, sides)),
            pltpu.SemaphoreType.DMA((ring, sides)),
            pltpu.SemaphoreType.DMA((chunks, sides)),
            pltpu.SemaphoreType.DMA((chunks, sides)),
            pltpu.SemaphoreType.DMA((4,)),
            pltpu.VMEM((ring, mine.shape[0], cross_q.shape[1]), jnp.bfloat16),
            pltpu.VMEM((ring, mine.shape[0], 2 * HD), jnp.float32),
            pltpu.VMEM((sides, mine.shape[0], width), jnp.bfloat16),
            pltpu.SemaphoreType.DMA((ring,)),
            pltpu.SemaphoreType.DMA((ring,)),
            pltpu.SemaphoreType.DMA((ring,)),
            pltpu.SemaphoreType.DMA((ring,)),
            pltpu.SemaphoreType.DMA((sides,)),
            pltpu.SemaphoreType.DMA((sides,)),
            pltpu.SemaphoreType.DMA((ring,)),
            pltpu.SemaphoreType.DMA((ring,)),
            pltpu.SemaphoreType.DMA((ring,)),
            pltpu.SemaphoreType.DMA((ring,)),
            pltpu.SemaphoreType.DMA((2,)),
        ],
        compiler_params=pltpu.CompilerParams(
            collective_id=1, has_side_effects=True, vmem_limit_bytes=50 * 1024 * 1024
        ),
        name="encoder_block",
    )(
        back, w_out, tokens, g_ffn[None, :], g_final[None, :], ffn_in, ffn_out, w_kv, cross_q, bias,
        w_cross, mine, live,
    )


def merge_tail(
    ring, sides, mixed, stats, w_ref, mine, live, decoded,
    got, got_stats, parts, ms, mr, ts, tr, ps, pr, ds, dr, fs, fr, ls,
):
    me = lax.axis_index("seq")
    here = lax.axis_index("head")
    rows, width = mine.shape
    mate = me + 1 - 2 * lax.rem(me, 2)

    def slab(owner):
        return pl.ds(pl.multiple_of(owner * rows, rows), rows)

    own_mixed = pltpu.make_async_copy(mixed.at[slab(me)], got.at[me], ls.at[0])
    own_stats = pltpu.make_async_copy(stats.at[slab(me)], got_stats.at[me], ls.at[1])
    own_mixed.start()
    own_stats.start()

    def copies(i, origin):
        to = lax.rem(me + i, ring)
        return (
            pltpu.make_async_remote_copy(
                src_ref=mixed.at[slab(to)],
                dst_ref=got.at[origin],
                send_sem=ms.at[i],
                recv_sem=mr.at[i],
                device_id={"seq": to},
                device_id_type=MESH,
            ),
            pltpu.make_async_remote_copy(
                src_ref=stats.at[slab(to)],
                dst_ref=got_stats.at[origin],
                send_sem=ts.at[i],
                recv_sem=tr.at[i],
                device_id={"seq": to},
                device_id_type=MESH,
            ),
        )

    def send(i, carry):
        for copy in copies(i, me):
            copy.start()
        return carry

    lax.fori_loop(1, ring, send, 0)

    def collect(i, carry):
        for copy in copies(i, lax.rem(me - i + ring, ring)):
            copy.wait()
        return carry

    lax.fori_loop(1, ring, collect, 0)
    own_mixed.wait()
    own_stats.wait()
    heads = w_ref.shape[0] // HD
    seen = got_stats[...]
    best = jnp.max(seen, axis=0, keepdims=True)
    grow = jnp.exp(seen - best)
    sums = pltpu.roll(seen.reshape(ring * rows, 2 * HD), HD, 1).reshape(ring, rows, 2 * HD)
    weight_sum = jnp.sum(grow * sums, axis=0, keepdims=True)
    factor = (grow / weight_sum).reshape(ring * rows, 2 * HD)
    lane = lax.broadcasted_iota(jnp.int32, (2 * HD, heads * HD), 1)
    row = lax.broadcasted_iota(jnp.int32, (2 * HD, heads * HD), 0)
    spread = jnp.where((lane >= row * HD) & (lane < row * HD + HD), 1.0, 0.0)
    factor = jnp.where(
        lax.broadcasted_iota(jnp.int32, factor.shape, 1) < heads, factor, 0.0
    )
    wide = jnp.dot(
        factor, spread, precision=lax.Precision.HIGHEST, preferred_element_type=jnp.float32
    ).reshape(ring, rows, heads * HD)
    context = jnp.sum(got[...].astype(jnp.float32) * wide, axis=0).astype(jnp.bfloat16)
    parts[here] = jnp.dot(context, w_ref[...], preferred_element_type=jnp.float32).astype(
        jnp.bfloat16
    )

    def swap(k, side):
        return side_copy(sides, k, parts.at[side], parts.at[side], ps.at[k], pr.at[k])

    for k in range(1, sides):
        swap(k, here).start()
    for k in range(1, sides):
        swap(k, here).wait_send()
        swap(k, lax.rem(here - k + sides, sides)).wait_recv()
    total = parts[0].astype(jnp.float32)
    for side in range(1, sides):
        total = total + parts[side].astype(jnp.float32)
    decoded[slab(me), :] = (
        mine[...].astype(jnp.float32) + jnp.where(live[...] > 0.0, total, 0.0)
    ).astype(jnp.bfloat16)

    def spread_out(j, owner):
        block = decoded.at[slab(owner)]
        return pltpu.make_async_remote_copy(
            src_ref=block,
            dst_ref=block,
            send_sem=ds.at[j],
            recv_sem=dr.at[j],
            device_id={"seq": lax.rem(me + 2 * j, ring)},
            device_id_type=MESH,
        )

    def hand_over(j, owner):
        block = decoded.at[slab(owner)]
        return pltpu.make_async_remote_copy(
            src_ref=block,
            dst_ref=block,
            send_sem=fs.at[j],
            recv_sem=fr.at[j],
            device_id={"seq": mate},
            device_id_type=MESH,
        )

    def share_out(j, carry):
        spread_out(j, me).start()
        return carry

    lax.fori_loop(1, ring // 2, share_out, 0)
    hand_over(0, me).start()

    def pass_on(j, carry):
        owner = lax.rem(me - 2 * j + ring, ring)
        spread_out(j, owner).wait_recv()
        hand_over(j, owner).start()
        return carry

    lax.fori_loop(1, ring // 2, pass_on, 0)

    def finish(j, carry):
        spread_out(j, me).wait_send()
        return carry

    lax.fori_loop(1, ring // 2, finish, 0)

    def drain(j, carry):
        hand_over(j, lax.rem(me - 2 * j + ring, ring)).wait_send()
        hand_over(j, lax.rem(mate - 2 * j + ring, ring)).wait_recv()
        return carry

    lax.fori_loop(0, ring // 2, drain, 0)


def project_kernel(share, tokens, gain, w_ref, q_out, kv_out):
    rows = tokens.shape[0]
    part = rows // share
    heads = w_ref.shape[2] // HD
    normed = norm_rows(tokens[...].astype(jnp.float32), gain[...]).astype(jnp.bfloat16)
    scaling = jnp.bfloat16(HD ** (-0.5))
    queries = (
        lax.dot_general(
            w_ref[0], normed, (((0,), (1,)), ((), ())), preferred_element_type=jnp.float32
        ).astype(jnp.bfloat16)
        * scaling
    )
    keys = jnp.dot(normed, w_ref[1], preferred_element_type=jnp.float32).astype(jnp.bfloat16)
    values = jnp.dot(normed, w_ref[2], preferred_element_type=jnp.float32).astype(jnp.bfloat16)
    for h in range(heads):
        cut = slice(h * HD, (h + 1) * HD)
        both = jnp.concatenate([keys[:, cut], values[:, cut]], axis=1)
        for s in range(share):
            at = slice(s * part, (s + 1) * part)
            q_out[h * share + s] = queries[cut, at]
            kv_out[h * share + s] = both[at, :]


def project_heads(share, tokens, gain, weights):
    rows = tokens.shape[0]
    heads = weights.shape[2] // HD
    part = rows // share
    vmem = pl.BlockSpec(memory_space=pltpu.VMEM)
    return pl.pallas_call(
        functools.partial(project_kernel, share),
        out_shape=(
            jax.ShapeDtypeStruct((heads * share, HD, part), jnp.bfloat16),
            jax.ShapeDtypeStruct((heads * share, part, 2 * HD), jnp.bfloat16),
        ),
        in_specs=[vmem, vmem, vmem],
        out_specs=(vmem, vmem),
        compiler_params=pltpu.CompilerParams(vmem_limit_bytes=40 * 1024 * 1024),
        name="project_heads",
    )(tokens, gain[None, :], weights)


def attend_kernel(lengths, q_ref, kv_ref, o_ref, keys, values, flipped, count):
    blocks, span, lanes = kv_ref.shape
    tile = span
    queries = q_ref.shape[1]
    group = math.gcd(queries, 256)
    ones_rows = flipped.shape[1] - HD
    lane = lax.broadcasted_iota(jnp.int32, (span, lanes), 1)
    row = lax.broadcasted_iota(jnp.int32, (span, lanes), 0)

    @pl.when(pl.program_id(0) == 0)
    def pack():
        def place(j, start):
            block = kv_ref[j]
            dead = jnp.where(row < lengths[j], 0.0, masked_score).astype(jnp.bfloat16)
            at = pl.ds(pl.multiple_of(start, 16), span)
            keys[at, :] = jnp.where(lane < HD, block, dead)
            values[at, :] = jnp.where(lane < HD, jnp.ones_like(block), block)
            return start + ((lengths[j] + 15) // 16) * 16

        stop = lax.fori_loop(0, blocks, place, 0)
        at = pl.ds(pl.multiple_of(stop, 16), span)
        keys[at, :] = jnp.where(lane < HD, 0.0, masked_score).astype(jnp.bfloat16)
        values[at, :] = jnp.zeros((span, lanes), jnp.bfloat16)
        count[0] = (stop + tile - 1) // tile

        def flip(t, carry):
            at = pl.ds(pl.multiple_of(t * tile, tile), tile)
            flipped[t] = values[at, :].T[HD - ones_rows :, :]
            return carry

        lax.fori_loop(0, count[0], flip, 0)

    spare = lax.broadcasted_iota(jnp.int32, (HD, queries), 0)
    pick = jnp.where(spare == 0, 1.0, 0.0).astype(jnp.bfloat16)
    q_wide = jnp.concatenate([q_ref[...], pick], axis=0)
    cuts = [slice(g, g + group) for g in range(0, queries, group)]

    def step(t, state):
        at = pl.ds(pl.multiple_of(t * tile, tile), tile)
        keys_here = keys[at, :]
        values_here = flipped[t]
        all_scores = [
            jnp.dot(keys_here, q_wide[:, cut], preferred_element_type=jnp.float32) for cut in cuts
        ]
        updated = []
        for scores, (top, mixed) in zip(all_scores, state):
            new_top = jnp.maximum(top, jnp.max(scores, axis=0, keepdims=True))
            weights = jnp.exp(scores - new_top).astype(jnp.bfloat16)
            part = jnp.dot(values_here, weights, preferred_element_type=jnp.float32)
            updated.append((new_top, mixed * jnp.exp(top - new_top) + part))
        return tuple(updated)

    start = tuple(
        (
            jnp.full((1, group), masked_score, jnp.float32),
            jnp.zeros((ones_rows + HD, group), jnp.float32),
        )
        for cut in cuts
    )
    ends = lax.fori_loop(0, count[0], step, start)
    for cut, (top, mixed) in zip(cuts, ends):
        o_ref[:, cut] = (mixed[ones_rows:, :] / mixed[0:1, :]).astype(jnp.bfloat16)


def attend(q_all, kv_all, pad_lengths):
    blocks, span, lanes = kv_all.shape
    total = q_all.shape[1]
    width = math.gcd(total, 2048)
    return pl.pallas_call(
        attend_kernel,
        out_shape=jax.ShapeDtypeStruct((HD, total), jnp.bfloat16),
        grid_spec=pltpu.PrefetchScalarGridSpec(
            num_scalar_prefetch=1,
            grid=(total // width,),
            in_specs=[
                pl.BlockSpec((HD, width), lambda i, lengths: (0, i)),
                pl.BlockSpec((blocks, span, lanes), lambda i, lengths: (0, 0, 0)),
            ],
            out_specs=pl.BlockSpec((HD, width), lambda i, lengths: (0, i)),
            scratch_shapes=[
                pltpu.VMEM(((blocks + 1) * span, lanes), jnp.bfloat16),
                pltpu.VMEM(((blocks + 1) * span, lanes), jnp.bfloat16),
                pltpu.VMEM((blocks + 1, HD + 16, span), jnp.bfloat16),
                pltpu.SMEM((1,), jnp.int32),
            ],
        ),
        compiler_params=pltpu.CompilerParams(
            dimension_semantics=("arbitrary",), vmem_limit_bytes=48 * 1024 * 1024
        ),
        name="attend",
    )(pad_lengths, q_all, kv_all)


def local(
    ring,
    sides,
    tokens,
    norm_attn,
    self_qkv,
    self_out,
    norm_ffn,
    ffn_in,
    ffn_out,
    norm_final,
    pad_lengths,
    targets,
    target_lengths,
    norm_cross,
    cross_query,
    cross_kv,
    cross_out,
):
    row_count = tokens.shape[0]
    heads_here = self_qkv.shape[2] // HD
    share = ring // heads_here
    part = row_count // share
    q_send, kv_send = project_heads(share, tokens, norm_attn, self_qkv)
    q_got, kv_got, out_all, cross_q = scatter_heads(
        ring, share, sides, q_send, kv_send, self_out, targets, norm_cross, cross_query
    )
    q_all = q_got.transpose(1, 0, 2).reshape(HD, ring * part)
    mixed_t = attend(q_all, kv_got, pad_lengths)
    back = mixed_t.reshape(HD, ring, part).transpose(1, 0, 2)
    my_length = lax.dynamic_slice_in_dim(pad_lengths, lax.axis_index("seq"), 1, 0)
    bias = jnp.where(
        jnp.arange(row_count, dtype=jnp.int32)[None, :] < my_length[0], 0.0, masked_score
    ).astype(jnp.float32)
    target_rows = targets.shape[0]
    slice_rows = target_rows // ring
    slots = lax.axis_index("seq") * slice_rows + jnp.arange(slice_rows, dtype=jnp.int32)
    owner = slots // TGT_LEN
    limits = jnp.sum(
        jnp.where(
            owner[:, None] == jnp.arange(target_lengths.shape[0])[None, :],
            target_lengths[None, :],
            0,
        ),
        axis=1,
    )
    target_live = slots % TGT_LEN < limits
    mine = lax.dynamic_slice_in_dim(targets, lax.axis_index("seq") * slice_rows, slice_rows, 0)
    live = jnp.broadcast_to(target_live[:, None], mine.shape).astype(jnp.float32)
    encoded, decoded = encoder_block(
        ring,
        share,
        sides,
        back,
        out_all.reshape(-1, out_all.shape[2]),
        tokens,
        norm_ffn,
        norm_final,
        ffn_in,
        ffn_out,
        cross_kv,
        cross_q,
        bias,
        cross_out,
        mine,
        live,
    )
    return (encoded, decoded)


def solution(mesh):
    ring = mesh.shape["seq"]
    sides = mesh.shape["head"]
    placed = (
        P("seq", None),
        P(),
        P(None, None, "head"),
        P("head", None),
        P(),
        P(None, None, "head"),
        P("head", None),
        P(),
        P(),
        P(),
        P(),
        P(),
        P(None, "head"),
        P(None, None, "head"),
        P("head", None),
    )
    return jax.shard_map(
        functools.partial(local, ring, sides),
        mesh=mesh,
        in_specs=placed,
        out_specs=(P("seq", None), P()),
        check_vma=False,
    )
```
